768 devices in a mesh: dp: 3 (over z_lo), context: 16 (over x, z_hi), tensor: 16 (over y, core).
Axes of the slice: x: 4, y: 8, z: 12 (z_hi: 4, z_lo: 3; z = z_hi * 3 + z_lo), core: 2. Of those that a mesh axis runs over, the one named last changes fastest.
Arguments:
- queries: bfloat16 [3, 4096, 8192], P('dp', 'context', 'tensor'), may hold values from -45 to 45
- keys: bfloat16 [3, 4096, 1024], P('dp', 'context'), may hold values from -20 to 20
- values: bfloat16 [3, 4096, 1024], P('dp', 'context'), may hold values from -6 to 6
- out_weight: bfloat16 [8192, 8192], P('tensor'), may hold values from -0.0625 to 0.0625
- segment_ids: int32 [3, 4096], P('dp'), may hold values from 0 to 7, as said below
- loss_mask: int32 [3, 4096], P('dp', 'context'), may hold values from 0 to 1, as said below
- span_order: int32 [32], replicated, may hold values from 0 to 31, as said below
Outputs:
- weighted_out: bfloat16 [3, 4096, 8192], P('dp', 'context', 'tensor')
The draws below stay inside these ranges and needn't reach their ends.
Inputs may be any that keep to these rules, and one draw needn't show every extreme that they name: `span_order`: a permutation of 0 .. 31. `segment_ids`: taken in order of sequence position pos (see the steps), a sequence's document numbers never fall; each sequence holds 8 documents. `loss_mask`: the first row of every sequence is 1.
All inputs are finite; a program needn't handle non-finite values.
Results may differ from the reference program's by a relative error of at most 0.018.
Values may be sent and summed in bfloat16 or wider, within the bound.
No kernel may reach another device: no remote copies, remote signals or barrier semaphores. Data moves between devices by JAX's collectives and lax.ppermute only.
A program may use at most 64 MiB of HBM per device.

```python
import jax
import jax.numpy as jnp
from jax import lax

D = 8192
QH = 64
KVH = 8
HD = 128
DOCS = 8
TOKENS = 4096
CH = 128
N_DP = 3
N_CONTEXT = 16
N_TENSOR = 16


def paired_heads(key):
    key_first = jax.random.fold_in(key, 11)
    query_first = jax.random.fold_in(key, 12)
    base_keys = jnp.clip(jax.random.normal(key_first, (N_DP, TOKENS, KVH, HD), jnp.float32), -6.0, 6.0)
    base_queries = jnp.clip(jax.random.normal(query_first, (N_DP, TOKENS, QH, HD), jnp.float32), -6.0, 6.0)
    keys_out = base_keys
    queries_out = base_queries
    return (queries_out.reshape(N_DP, TOKENS, QH * HD), keys_out.reshape(N_DP, TOKENS, KVH * HD))


def draw_queries(key, part):
    return paired_heads(key)[0].astype(jnp.bfloat16)


def draw_keys(key, part):
    return paired_heads(key)[1].astype(jnp.bfloat16)


def document_cuts(cut_key):
    chosen = jax.random.permutation(cut_key, TOKENS - 1)[:DOCS - 1].astype(jnp.int32) + 1
    return jnp.zeros((TOKENS,), jnp.int32).at[chosen].set(1)


def layout_tables(key):
    order = jax.random.permutation(jax.random.fold_in(key, 21), 2 * N_CONTEXT).astype(jnp.int32)
    replica_keys = jax.random.split(jax.random.fold_in(key, 22), N_DP)
    starts = jax.vmap(document_cuts)(replica_keys)
    ordered = jnp.cumsum(starts, axis=1).astype(jnp.int32)
    rows = jnp.arange(TOKENS, dtype=jnp.int32)
    position = order[rows // CH] * CH + rows % CH
    return (order, ordered[:, position])


def draw_span_order(key, part):
    return layout_tables(key)[0]


def draw_segment_ids(key, part):
    return layout_tables(key)[1]


def draw_loss_mask(key, part):
    replica = jnp.arange(N_DP, dtype=jnp.int32)[:, None]
    rows = jnp.arange(TOKENS, dtype=jnp.int32)[None, :]
    limit = 150 + 350 * replica // max(N_DP - 1, 1) + 350 * rows // TOKENS
    rolls = jax.random.randint(key, (N_DP, TOKENS), 0, 1000)
    marked = (rolls < limit).astype(jnp.int32)
    return marked.at[:, 0].set(1)


def levels(own_key, shape, cuts, low, largest):
    def one(dim, parts):
        heights = jax.random.uniform(jax.random.fold_in(jax.random.fold_in(own_key, 6), dim), (parts,), jnp.float32, low / len(cuts), largest / len(cuts))
        return jnp.repeat(jnp.exp(heights), shape[dim] // parts).reshape((-1,) + (1,) * (len(shape) - dim - 1))

    gain = one(*cuts[0])
    for cut in cuts[1:]:
        gain = gain * one(*cut)
    return gain


def noise(stream_key, dims, scale, bound, cuts=(), held_as=jnp.bfloat16):
    level = levels(stream_key, dims, cuts, -0.22, 0.18) if cuts else 1.0
    result = jax.random.normal(stream_key, dims, jnp.float32) * scale * level
    return jnp.minimum(jnp.maximum(result, -bound), bound).astype(held_as)


def setup_inputs(seed: int = 0) -> dict:
    key_list = jax.random.split(jax.random.key(seed), 8)
    queries = draw_queries(jax.random.fold_in(key_list[7], 71), 0)
    keys = draw_keys(jax.random.fold_in(key_list[7], 71), 0)
    values = noise(key_list[2], (N_DP, TOKENS, KVH * HD), 1.0, 6.0, ((0, 3), (1, 16)))
    out_weight = noise(key_list[3], (QH * HD, D), (QH * HD) ** -0.5, 0.0625, ((0, 16),))
    segment_ids = draw_segment_ids(jax.random.fold_in(key_list[7], 71), 0)
    loss_mask = draw_loss_mask(jax.random.fold_in(key_list[7], 71), 0)
    span_order = draw_span_order(jax.random.fold_in(key_list[7], 71), 0)
    return {"queries": queries, "keys": keys, "values": values, "out_weight": out_weight, "segment_ids": segment_ids, "loss_mask": loss_mask, "span_order": span_order}


def reference(queries, keys, values, out_weight, segment_ids, loss_mask, span_order):
    rows = jnp.arange(TOKENS, dtype=jnp.int32)
    position = span_order[rows // CH] * CH + rows % CH
    group = QH // KVH
    width = QH * HD // N_TENSOR
    factor = HD ** -0.5
    count = jnp.sum(loss_mask.astype(jnp.float32))
    results = []
    for replica in range(N_DP):
        segment = segment_ids[replica]
        allowed = (segment[:, None] == segment[None, :]) & (position[:, None] >= position[None, :])
        query_all = queries[replica]
        key_all = keys[replica]
        value_all = values[replica]

        def one_head(head):
            query = lax.dynamic_slice_in_dim(query_all, (head * HD).astype(jnp.int32), HD, 1)
            kv_start = ((head // group) * HD).astype(jnp.int32)
            key_head = lax.dynamic_slice_in_dim(key_all, kv_start, HD, 1)
            value_head = lax.dynamic_slice_in_dim(value_all, kv_start, HD, 1)
            scores = jnp.dot(query, key_head.T, preferred_element_type=jnp.float32) * factor
            scores = jnp.where(allowed, scores, -1e30)
            best = jnp.max(scores, axis=-1, keepdims=True)
            probs = jnp.where(allowed, jnp.exp(scores - best), 0.0)
            total = jnp.sum(probs, axis=-1, keepdims=True)
            mixed = jnp.dot(probs.astype(jnp.bfloat16), value_head, preferred_element_type=jnp.float32) / total
            return mixed.astype(jnp.bfloat16)

        heads = lax.map(one_head, jnp.arange(QH, dtype=jnp.int32))
        joined = jnp.transpose(heads, (1, 0, 2)).reshape(TOKENS, QH * HD)
        summed = jnp.zeros((TOKENS, D), jnp.float32)
        for member in range(N_TENSOR):
            partial_value = jnp.dot(joined[:, member * width:(member + 1) * width], out_weight[member * width:(member + 1) * width], preferred_element_type=jnp.float32)
            rounded = lax.optimization_barrier(partial_value.astype(jnp.bfloat16))
            summed = summed + rounded.astype(jnp.float32)
        weight = loss_mask[replica].astype(jnp.float32) * (N_DP * TOKENS) / count
        results.append((summed * weight[:, None]).astype(jnp.bfloat16))
    return jnp.stack(results)
```

```python
import functools

import jax
import jax.numpy as jnp
import numpy as np
from jax import lax
from jax.experimental import pallas as pl
from jax.experimental.pallas import tpu as pltpu
from jax.sharding import PartitionSpec as P

HD = 128
SPAN = 128
LOG2E = 1.4426950408889634


NX, NZ, NY, NC = 4, 4, 8, 2


def inner(i, c, n):
    return ((((i - c) % n) ^ 1) + c) % n


def outer(i, c, n):
    v = (i - c) % n
    return (v + (1 if v % 2 else -1) + c) % n


def perm_context(axis, partner):
    out = []
    for x in range(NX):
        for z in range(NZ):
            for y in range(NY):
                for c in range(NC):
                    px = partner(x, c, NX) if axis == "x" else x
                    pz = partner(z, c, NZ) if axis == "z" else z
                    tensor = y * NC + c
                    out.append(((x * NZ + z) * 16 + tensor, (px * NZ + pz) * 16 + tensor))
    return out


def perm_tensor(partner):
    return [
        (y * NC + c, partner(y, c, NY) * NC + c) for y in range(NY) for c in range(NC)
    ]


SWAP = [(t, t ^ 1) for t in range(16)]


def slot_table():
    table = np.zeros((16, NC, 32), np.int32)
    for x in range(NX):
        for z in range(NZ):
            for c in range(NC):
                rows = []
                for core in (c, 1 - c):
                    zs = [z, inner(z, core, NZ)]
                    zs += [outer(z, core, NZ), inner(outer(z, core, NZ), core, NZ)]
                    xs = [x, inner(x, core, NX)]
                    xs += [outer(x, core, NX), inner(outer(x, core, NX), core, NX)]
                    rows += [2 * (xx * NZ + zz) + core for xx in xs for zz in zs]
                table[x * NZ + z, c] = rows
    return table


def block_table():
    table = np.zeros((16, 8), np.int32)
    for y in range(NY):
        for c in range(NC):
            v = (y - c) % NY
            k, s = v // 2, v % 2
            far = (k + 2) % 4
            mid = (k + 1 - 2 * s) % 4
            near = (k - 1 + 2 * s) % 4
            order = [2 * far + s, 2 * far + 1 - s]
            order += [2 * mid + 1 - s, 2 * mid + s]
            order += [2 * near + s, 2 * near + 1 - s]
            order += [2 * k + 1 - s, 2 * k + s]
            table[y * NC + c] = [2 * ((b + c) % NY) + c for b in order]
    return table


CHUNK = 256
PAD = CHUNK // SPAN - 1


def attention_kernel(info, lo_ref, q_ref, a_ref, b_ref, c_ref, d_ref, out_ref, kv, q4, m_ref, l_ref, acc):
    n_spans = 32
    heads = q_ref.shape[1] // HD
    kv[: PAD * SPAN, :] = jnp.zeros((PAD * SPAN, 2 * HD), kv.dtype)
    for which, ref in enumerate((a_ref, b_ref, c_ref, d_ref)):
        for i in range(8):
            at = pl.multiple_of((info[which * 8 + i] + PAD) * SPAN, SPAN)
            kv[pl.ds(at, SPAN), :] = ref[i * SPAN : (i + 1) * SPAN, :]
    scale = HD ** (-0.5) * LOG2E
    width = heads * SPAN
    for i in range(2):
        for h in range(heads):
            q4[h * SPAN : (h + 1) * SPAN, :] = q_ref[i * SPAN : (i + 1) * SPAN, h * HD : (h + 1) * HD]
        q_pos = info[n_spans + i]
        first = info[n_spans + 2 + i]
        lo = jnp.concatenate([lo_ref[i : i + 1, :]] * heads, axis=1)
        lane = lax.broadcasted_iota(jnp.int32, (1, SPAN), 1) + q_pos * SPAN
        hi = jnp.concatenate([lane] * heads, axis=1)
        m_ref[...] = jnp.full((1, width), -1e30, jnp.float32)
        l_ref[...] = jnp.zeros((1, width), jnp.float32)
        acc[...] = jnp.zeros((HD, width), jnp.float32)
        count = lax.div((q_pos + 1) * SPAN - first + CHUNK - 1, CHUNK)

        def step(j, carry):
            start = (q_pos + 1) * SPAN - (j + 1) * CHUNK
            at = pl.multiple_of(start + PAD * SPAN, SPAN)
            k = kv[pl.ds(at, CHUNK), :HD]
            v = kv[pl.ds(at, CHUNK), HD:]
            s = lax.dot_general(k, q4[...], (((1,), (1,)), ((), ())), preferred_element_type=jnp.float32)
            pos = lax.broadcasted_iota(jnp.int32, (CHUNK, width), 0) + start
            s = jnp.where((pos >= lo) & (pos <= hi), s * scale, -1e30)
            old = m_ref[...]
            new = jnp.maximum(old, jnp.max(s, axis=0, keepdims=True))
            alpha = jnp.exp2(old - new)
            p = jnp.exp2(s - new)
            m_ref[...] = new
            l_ref[...] = l_ref[...] * alpha + jnp.sum(p, axis=0, keepdims=True)
            add = lax.dot_general(
                v, p.astype(jnp.bfloat16), (((0,), (0,)), ((), ())), preferred_element_type=jnp.float32
            )
            acc[...] = acc[...] * alpha + add
            return carry

        lax.fori_loop(0, count, step, 0)
        result = acc[...] / l_ref[...]
        for h in range(heads):
            out_ref[i * SPAN : (i + 1) * SPAN, h * HD : (h + 1) * HD] = result[
                :, h * SPAN : (h + 1) * SPAN
            ].T.astype(jnp.bfloat16)


def attention(info, lo, q, parts):
    rows, width = q.shape
    vmem = pl.BlockSpec(memory_space=pltpu.VMEM)
    return pl.pallas_call(
        attention_kernel,
        out_shape=jax.ShapeDtypeStruct((rows, width), jnp.bfloat16),
        in_specs=[pl.BlockSpec(memory_space=pltpu.SMEM)] + [vmem] * 6,
        out_specs=vmem,
        scratch_shapes=[
            pltpu.VMEM(((32 + PAD) * SPAN, 2 * HD), jnp.bfloat16),
            pltpu.VMEM((width // HD * SPAN, HD), jnp.bfloat16),
            pltpu.VMEM((1, width // HD * SPAN), jnp.float32),
            pltpu.VMEM((1, width // HD * SPAN), jnp.float32),
            pltpu.VMEM((HD, width // HD * SPAN), jnp.float32),
        ],
        name="attend",
    )(info, lo, q, *parts)


def project_kernel(order, mine_ref, other_ref, w_ref, w_other_ref, out_ref):
    total = jnp.dot(mine_ref[...], w_ref[...], preferred_element_type=jnp.float32)
    total += jnp.dot(other_ref[...], w_other_ref[...], preferred_element_type=jnp.float32)
    out_ref[0] = total.astype(jnp.bfloat16)


def project(order, first, count, part, mine, other, w, w_other):
    depth = w.shape[0]
    cols = 512
    rows = SPAN
    pick = lambda g, order: (0, order[first + g])
    return pl.pallas_call(
        project_kernel,
        out_shape=jax.ShapeDtypeStruct((count, rows, cols), jnp.bfloat16),
        grid_spec=pltpu.PrefetchScalarGridSpec(
            num_scalar_prefetch=1,
            grid=(count,),
            in_specs=[
                pl.BlockSpec((rows, depth), lambda g, order: (part, 0)),
                pl.BlockSpec((rows, depth), lambda g, order: (part, 0)),
                pl.BlockSpec((depth, cols), pick),
                pl.BlockSpec((depth, cols), pick),
            ],
            out_specs=pl.BlockSpec((1, rows, cols), lambda g, order: (g, 0, 0)),
        ),
        name="project",
    )(order, mine, other, w, w_other)


def add(a, b):
    return (a.astype(jnp.float32) + b.astype(jnp.float32)).astype(jnp.bfloat16)


def per_device(queries, keys, values, out_weight, segment_ids, loss_mask, span_order):
    tensor = lax.axis_index("tensor")
    context = lax.axis_index("context")
    y, core = tensor // NC, tensor % NC
    both = ("context", "tensor")

    weight_other = lax.ppermute(out_weight, "tensor", SWAP)

    take = lambda a: lax.dynamic_slice(a[0], (core * SPAN, y * HD), (SPAN, HD))
    kv1 = jnp.concatenate([take(keys), take(values)], axis=1)
    r1 = lax.ppermute(kv1, both, perm_context("z", inner))
    kv2 = jnp.concatenate([kv1, r1], axis=0)
    r2 = lax.ppermute(kv2, both, perm_context("z", outer))
    kv4 = jnp.concatenate([kv2, r2], axis=0)
    r4 = lax.ppermute(kv4, both, perm_context("x", inner))
    kv8 = jnp.concatenate([kv4, r4], axis=0)
    r8 = lax.ppermute(kv8, both, perm_context("x", outer))
    o8 = lax.ppermute(kv8, "tensor", SWAP)
    p8 = lax.ppermute(r8, "tensor", SWAP)

    slots = lax.dynamic_slice(
        jnp.asarray(slot_table()), (context, core, 0), (1, 1, 32)
    ).reshape(32)
    place = jnp.sum(
        jnp.where(slots[:, None] == jnp.arange(32, dtype=jnp.int32)[None, :], span_order[None, :], 0), axis=1
    )
    q_pos = lax.dynamic_slice(span_order, (2 * context,), (2,))
    seg = segment_ids[0]
    q_seg = lax.dynamic_slice(seg, (context * 2 * SPAN,), (2 * SPAN,))
    lo = jnp.sum((seg[None, :] < q_seg[:, None]).astype(jnp.int32), axis=1).reshape(2, SPAN)
    info = jnp.concatenate([place, q_pos, lo[:, 0]])

    heads = attention(info, lo, queries[0], (kv8, r8, o8, p8))
    heads_other = lax.ppermute(heads, "tensor", SWAP)

    order = lax.dynamic_slice(jnp.asarray(block_table()), (tensor, 0), (1, 8)).reshape(8)

    count = jnp.sum(loss_mask[0].astype(jnp.float32)) * jnp.ones((8, 128), jnp.float32)
    for d in (1, 2):
        count = count + lax.ppermute(count, "context", [(i, i ^ d) for i in range(16)])
    for d in (4, 8):
        count = count + lax.ppermute(count, "context", [(i, i ^ d) for i in range(16)])
    one = lax.ppermute(count, "dp", [(i, (i + 1) % 3) for i in range(3)])
    two = lax.ppermute(count, "dp", [(i, (i + 2) % 3) for i in range(3)])
    count = (count + one + two)[0, 0]
    scale_all = lax.axis_size("dp") * lax.axis_size("context") * queries.shape[1]
    weight = loss_mask[0].astype(jnp.float32) * scale_all / count

    inward, outward = perm_tensor(inner), perm_tensor(outer)
    results = []
    for part in range(2):
        args = (part, heads, heads_other, out_weight, weight_other)
        far = project(order, 0, 2, *args)
        far = lax.ppermute(far, "tensor", outward)
        rest = project(order, 2, 6, *args)
        mid = lax.ppermute(add(rest[0:2], far), "tensor", inward)
        near = lax.ppermute(add(rest[2:4], mid), "tensor", outward)
        last = lax.ppermute(add(rest[4], near[0]), "tensor", inward)
        f32 = jnp.float32
        summed = rest[5].astype(f32) + near[1].astype(f32) + last.astype(f32)
        rows = weight[part * SPAN : (part + 1) * SPAN]
        results.append((summed * rows[:, None]).astype(jnp.bfloat16))
    return jnp.concatenate(results, axis=0)[None]


def solution(mesh):
    in_specs = (
        P("dp", "context", "tensor"),
        P("dp", "context", None),
        P("dp", "context", None),
        P("tensor", None),
        P("dp", None),
        P("dp", "context"),
        P(),
    )
    out_specs = P("dp", "context", "tensor")
    return jax.shard_map(
        per_device, mesh=mesh, in_specs=in_specs, out_specs=out_specs, check_vma=False
    )
```

```python
import functools

import jax
import jax.numpy as jnp
import numpy as np
from jax import lax
from jax.experimental import pallas as pl
from jax.experimental.pallas import tpu as pltpu
from jax.sharding import PartitionSpec as P

HD = 128
SPAN = 128
TALLY = 8
BLOCK = SPAN + TALLY
COLS = 512
LOG2E = 1.4426950408889634
LOW = -1e30


NX, NZ, NY, NC = 4, 4, 8, 2


def inner(i, c, n):
    return ((((i - c) % n) ^ 1) + c) % n


def outer(i, c, n):
    v = (i - c) % n
    return (v + (1 if v % 2 else -1) + c) % n


def perm_context(axis, partner):
    out = []
    for x in range(NX):
        for z in range(NZ):
            for y in range(NY):
                for c in range(NC):
                    px = partner(x, c, NX) if axis == "x" else x
                    pz = partner(z, c, NZ) if axis == "z" else z
                    tensor = y * NC + c
                    out.append(((x * NZ + z) * 16 + tensor, (px * NZ + pz) * 16 + tensor))
    return out


def perm_tensor(partner):
    return [
        (y * NC + c, partner(y, c, NY) * NC + c) for y in range(NY) for c in range(NC)
    ]


SWAP = [(t, t ^ 1) for t in range(16)]


def slot_table():
    table = np.zeros((16, NC, 16), np.int32)
    for x in range(NX):
        for z in range(NZ):
            for c in range(NC):
                far = outer(z, c, NZ)
                rows = []
                for zs in ((z, inner(z, c, NZ)), (far, inner(far, c, NZ))):
                    rows += [2 * (xx * NZ + zz) + c for xx in range(NX) for zz in zs]
                table[x * NZ + z, c] = rows
    return table


def block_table():
    table = np.zeros((16, 8), np.int32)
    for y in range(NY):
        for c in range(NC):
            v = (y - c) % NY
            k, s = v // 2, v % 2
            far = (k + 2) % 4
            mid = (k + 1 - 2 * s) % 4
            near = (k - 1 + 2 * s) % 4
            order = [2 * far + s, 2 * far + 1 - s]
            order += [2 * mid + 1 - s, 2 * mid + s]
            order += [2 * near + s, 2 * near + 1 - s]
            order += [2 * k + 1 - s, 2 * k + s]
            table[y * NC + c] = [2 * ((b + c) % NY) + c for b in order]
    return table


SMEM = pl.BlockSpec(memory_space=pltpu.SMEM)
VMEM = pl.BlockSpec(memory_space=pltpu.VMEM)
HBM = pl.BlockSpec(memory_space=pltpu.HBM)


def grant(mib):
    return pltpu.CompilerParams(vmem_limit_bytes=mib * 2**20)


def prepare_kernel(k_ref, v_ref, mask_ref, out_ref, sems):
    tensor = lax.axis_index("tensor")
    rows = pl.ds(pl.multiple_of(lax.rem(tensor, NC) * SPAN, SPAN), SPAN)
    cols = pl.ds(pl.multiple_of(lax.div(tensor, NC) * HD, HD), HD)
    copies = []
    for i, ref in enumerate((k_ref, v_ref)):
        into = out_ref.at[pl.ds(0, SPAN), pl.ds(i * HD, HD)]
        copies.append(pltpu.make_async_copy(ref.at[0, rows, cols], into, sems.at[i]))
        copies[-1].start()
    total = jnp.sum(mask_ref[...].astype(jnp.float32), axis=1, keepdims=True)
    out_ref[SPAN:, :] = jnp.broadcast_to(total, (TALLY, 2 * HD)).astype(jnp.bfloat16)
    for copy in copies:
        copy.wait()


def prepare(keys, values, loss_mask):
    return pl.pallas_call(
        prepare_kernel,
        out_shape=jax.ShapeDtypeStruct((BLOCK, 2 * HD), jnp.bfloat16),
        in_specs=[HBM, HBM, VMEM],
        out_specs=VMEM,
        scratch_shapes=[pltpu.SemaphoreType.DMA((2,))],
        compiler_params=grant(2),
        name="prepare",
    )(keys, values, loss_mask)


def pack_kernel(order, w_ref, out_ref, sems):
    other = (lax.axis_index("tensor") ^ 1) * 8
    copies = []
    for g in range(8):
        at = pl.multiple_of(order[other + g] * COLS, COLS)
        copies.append(pltpu.make_async_copy(w_ref.at[:, pl.ds(at, COLS)], out_ref.at[g], sems.at[g]))
        copies[-1].start()
    for copy in copies:
        copy.wait()


def pack(order, w):
    return pl.pallas_call(
        pack_kernel,
        out_shape=jax.ShapeDtypeStruct((8, w.shape[0], COLS), w.dtype),
        in_specs=[SMEM, HBM],
        out_specs=HBM,
        scratch_shapes=[pltpu.SemaphoreType.DMA((8,))],
        compiler_params=grant(2),
        name="pack",
    )(order, w)


def attention_kernel(
    slots, spans, seg_ref, q_ref, q_other_ref, a_ref, b_ref, out_ref, tally_ref, kv, q8, items, lo_ref, m_ref, l_ref, acc
):
    f32 = jnp.float32
    context = lax.axis_index("context")
    core = lax.rem(lax.axis_index("tensor"), NC)
    heads = 2 * q_ref.shape[1] // HD
    half = heads // 2
    width = heads * SPAN
    tally = jnp.zeros((TALLY, HD), f32)
    for which, ref in enumerate((a_ref, b_ref)):
        for i in range(8):
            kv[which * 8 + i] = ref[i * BLOCK : i * BLOCK + SPAN, :]
            tally += ref[i * BLOCK + SPAN : (i + 1) * BLOCK, :HD].astype(f32)
    tally_ref[...] = tally
    seg = seg_ref[...]
    starts = [jnp.sum((seg < d).astype(f32), keepdims=True) for d in range(1, 8)]
    base = (context * NC + core) * 16
    count = jnp.int32(0)
    for i in range(2):
        for h in range(heads):
            ref = q_ref if h < half else q_other_ref
            q8[i, h * SPAN : (h + 1) * SPAN, :] = ref[i * SPAN : (i + 1) * SPAN, h % half * HD : (h % half + 1) * HD]
        q_seg = seg_ref[pl.ds(2 * context + i, 1), :]
        lo = jnp.zeros((1, SPAN), f32)
        for d in range(1, 8):
            lo = jnp.where(q_seg == d, starts[d - 1], lo)
        lo_ref[i] = lo
        first = jnp.min(lo).astype(jnp.int32)
        q_pos = spans[2 * context + i]
        m_ref[i] = jnp.full((1, width), LOW, f32)
        l_ref[i] = jnp.zeros((1, width), f32)
        acc[i] = jnp.zeros((HD, width), f32)
        for b in range(16):
            pos = spans[slots[base + b]]
            items[count] = i * 16 + b
            seen = (pos <= q_pos) & ((pos + 1) * SPAN > first)
            count = count + seen.astype(jnp.int32)

    def step(j, carry):
        item = items[j]
        i, b = lax.shift_right_logical(item, 4), item & 15
        pos = lax.broadcasted_iota(jnp.int32, (SPAN, SPAN), 0) + spans[slots[base + b]] * SPAN
        hi = lax.broadcasted_iota(jnp.int32, (SPAN, SPAN), 1) + spans[2 * context + i] * SPAN
        bias = jnp.where((pos.astype(f32) >= lo_ref[i]) & (pos <= hi), 0.0, LOW)
        s = lax.dot_general(kv[b, :, :HD], q8[i], (((1,), (1,)), ((), ())), preferred_element_type=f32)
        s = s * (HD ** (-0.5) * LOG2E) + jnp.concatenate([bias] * heads, axis=1)
        old = m_ref[i]
        new = jnp.maximum(old, jnp.max(s, axis=0, keepdims=True))
        alpha = jnp.exp2(old - new)
        p = jnp.exp2(s - new)
        m_ref[i] = new
        l_ref[i] = l_ref[i] * alpha + jnp.sum(p, axis=0, keepdims=True)
        add = lax.dot_general(
            kv[b, :, HD:], p.astype(jnp.bfloat16), (((0,), (0,)), ((), ())), preferred_element_type=f32
        )
        acc[i] = acc[i] * alpha + add
        return carry

    lax.fori_loop(0, count, step, 0)
    row = lax.broadcasted_iota(jnp.int32, (TALLY, width), 0)
    for i in range(2):
        cols = slice(i * width, (i + 1) * width)
        total = l_ref[i]
        total = jnp.where(total > 0, total, 1.0)
        out_ref[:SPAN, cols] = (acc[i] / total).astype(jnp.bfloat16)
        log = m_ref[i] + jnp.log(total) * LOG2E
        high = log.astype(jnp.bfloat16).astype(f32)
        mid = (log - high).astype(jnp.bfloat16).astype(f32)
        tail = log - high - mid
        parts = jnp.where(row == 0, high, jnp.where(row == 1, mid, jnp.where(row == 2, tail, 0.0)))
        out_ref[SPAN:, cols] = parts.astype(jnp.bfloat16)


def attention(slots, spans, seg, q, q_other, a, b):
    heads = 2 * q.shape[1] // HD
    width = heads * SPAN
    return pl.pallas_call(
        attention_kernel,
        out_shape=(
            jax.ShapeDtypeStruct((BLOCK, 2 * width), jnp.bfloat16),
            jax.ShapeDtypeStruct((TALLY, HD), jnp.float32),
        ),
        in_specs=[SMEM, SMEM] + [VMEM] * 5,
        out_specs=(VMEM, VMEM),
        scratch_shapes=[
            pltpu.VMEM((16, SPAN, 2 * HD), jnp.bfloat16),
            pltpu.VMEM((2, width, HD), jnp.bfloat16),
            pltpu.SMEM((33,), jnp.int32),
            pltpu.VMEM((2, 1, SPAN), jnp.float32),
            pltpu.VMEM((2, 1, width), jnp.float32),
            pltpu.VMEM((2, 1, width), jnp.float32),
            pltpu.VMEM((2, HD, width), jnp.float32),
        ],
        compiler_params=grant(12),
        name="attend",
    )(slots, spans, seg, q, q_other, a, b)


def multiply(order, first, heads_ref, w_ref, other_ref, out_ref):
    depth = w_ref.shape[0]
    mine = lax.axis_index("tensor") * 8
    for g in range(out_ref.shape[0]):
        at = pl.multiple_of(order[mine + first + g] * COLS, COLS)
        total = jnp.dot(heads_ref[:, :depth], w_ref[:, pl.ds(at, COLS)], preferred_element_type=jnp.float32)
        total += jnp.dot(heads_ref[:, depth:], other_ref[first + g], preferred_element_type=jnp.float32)
        out_ref[g] = total.astype(jnp.bfloat16)


def join_kernel(order, mine_ref, theirs_ref, w_ref, other_ref, heads_ref, out_ref):
    f32 = jnp.float32
    width = mine_ref.shape[1] // 2
    heads = width // SPAN

    def log(ref, at):
        rows = ref[SPAN:, at : at + SPAN].astype(f32)
        return rows[0:1] + rows[1:2] + rows[2:3]

    for i in range(2):
        for h in range(heads):
            a = i * width + h * SPAN
            b = i * width + (h + heads // 2) % heads * SPAN
            log_a, log_b = log(mine_ref, a), log(theirs_ref, b)
            top = jnp.maximum(log_a, log_b)
            part_a, part_b = jnp.exp2(log_a - top), jnp.exp2(log_b - top)
            total = part_a + part_b
            joined = mine_ref[:SPAN, a : a + SPAN].astype(f32) * (part_a / total)
            joined += theirs_ref[:SPAN, b : b + SPAN].astype(f32) * (part_b / total)
            heads_ref[i * SPAN : (i + 1) * SPAN, h * HD : (h + 1) * HD] = joined.T.astype(jnp.bfloat16)
    multiply(order, 0, heads_ref, w_ref, other_ref, out_ref)


def join(order, mine, theirs, w, other):
    rows, depth = 2 * SPAN, 2 * w.shape[0]
    return pl.pallas_call(
        join_kernel,
        out_shape=(
            jax.ShapeDtypeStruct((rows, depth), jnp.bfloat16),
            jax.ShapeDtypeStruct((2, rows, COLS), jnp.bfloat16),
        ),
        in_specs=[SMEM] + [VMEM] * 4,
        out_specs=(VMEM, VMEM),
        compiler_params=grant(20),
        name="join",
    )(order, mine, theirs, w, other)


def project_kernel(order, heads_ref, w_ref, other_ref, out_ref):
    multiply(order, 2, heads_ref, w_ref, other_ref, out_ref)


def project(order, heads, w, other):
    rows = heads.shape[0]
    return pl.pallas_call(
        project_kernel,
        out_shape=jax.ShapeDtypeStruct((6, rows, COLS), jnp.bfloat16),
        in_specs=[SMEM] + [VMEM] * 3,
        out_specs=VMEM,
        compiler_params=grant(20),
        name="project",
    )(order, heads, w, other)


def add(a, b):
    return (a.astype(jnp.float32) + b.astype(jnp.float32)).astype(jnp.bfloat16)


def per_device(queries, keys, values, out_weight, segment_ids, loss_mask, span_order):
    both = ("context", "tensor")
    f32 = jnp.float32
    cat = lambda *a: jnp.concatenate(a, axis=0)
    order = jnp.asarray(block_table().reshape(-1))
    slots = jnp.asarray(slot_table().reshape(-1))
    along_x = [[x * NZ + z for x in range(NX)] for z in range(NZ)]
    gather = lambda a: lax.all_gather(a, "context", axis=0, tiled=True, axis_index_groups=along_x)

    in_hbm = lambda a: pltpu.with_memory_space_constraint(a, pltpu.HBM)
    kv1 = prepare(in_hbm(keys), in_hbm(values), loss_mask)
    r1 = lax.ppermute(kv1, both, perm_context("z", inner))
    q_other = lax.ppermute(queries[0], "tensor", SWAP)
    packed = pack(order, in_hbm(out_weight))
    r1, packed = lax.optimization_barrier((r1, packed))
    kv2 = cat(kv1, r1)
    r2 = lax.ppermute(kv2, both, perm_context("z", outer))
    weight_other = lax.ppermute(packed, "tensor", SWAP)
    near = gather(kv2)
    far = gather(r2)
    mine, tally = attention(slots, span_order, segment_ids.reshape(32, SPAN), queries[0], q_other, near, far)
    theirs = lax.ppermute(mine, "tensor", SWAP)

    inward, outward = perm_tensor(inner), perm_tensor(outer)
    heads, far = join(order, mine, theirs, out_weight, weight_other)
    far = lax.ppermute(far, "tensor", outward)
    rest = project(order, heads, out_weight, weight_other)
    rest, tally = lax.optimization_barrier((rest, tally))
    around = [(d * 16 + t, (d + 1 + t % 2) % 3 * 16 + t) for d in range(3) for t in range(16)]
    one = lax.ppermute(tally, ("dp", "tensor"), around)
    mid = lax.ppermute(add(rest[0:2], far), "tensor", inward)
    two = lax.ppermute(one, "tensor", SWAP)
    near = lax.ppermute(add(rest[2:4], mid), "tensor", outward)
    last = lax.ppermute(add(rest[4], near[0]), "tensor", inward)
    count = (tally + one + two)[0, 0]
    scale_all = lax.axis_size("dp") * lax.axis_size("context") * queries.shape[1]
    weight = loss_mask[0].astype(f32) * scale_all / count
    summed = rest[5].astype(f32) + near[1].astype(f32) + last.astype(f32)
    return (summed * weight[:, None]).astype(jnp.bfloat16)[None]


def solution(mesh):
    in_specs = (
        P("dp", "context", "tensor"),
        P("dp", "context", None),
        P("dp", "context", None),
        P("tensor", None),
        P("dp", None),
        P("dp", "context"),
        P(),
    )
    out_specs = P("dp", "context", "tensor")
    return jax.shard_map(
        per_device, mesh=mesh, in_specs=in_specs, out_specs=out_specs, check_vma=False
    )
```

```python
import jax
import jax.numpy as jnp
import numpy as np
from jax import lax
from jax.experimental import pallas as pl
from jax.experimental.pallas import tpu as pltpu
from jax.sharding import PartitionSpec as P


HD = 128
SPAN = 128
TALLY = 8
BLOCK = SPAN + TALLY
COLS = 512
LOG2E = 1.4426950408889634
LOW = -1e30


NX, NZ, NY, NC = 4, 4, 8, 2


def inner(i, c, n):
    return ((((i - c) % n) ^ 1) + c) % n


def outer(i, c, n):
    v = (i - c) % n
    return (v + (1 if v % 2 else -1) + c) % n


def perm_context(axis, partner):
    out = []
    for x in range(NX):
        for z in range(NZ):
            for y in range(NY):
                for c in range(NC):
                    px = partner(x, c, NX) if axis == "x" else x
                    pz = partner(z, c, NZ) if axis == "z" else z
                    tensor = y * NC + c
                    out.append(((x * NZ + z) * 16 + tensor, (px * NZ + pz) * 16 + tensor))
    return out


def perm_tensor(partner):
    return [
        (y * NC + c, partner(y, c, NY) * NC + c) for y in range(NY) for c in range(NC)
    ]


SWAP = [(t, t ^ 1) for t in range(16)]


def slot_table():
    table = np.zeros((16, NC, 16), np.int32)
    for x in range(NX):
        for z in range(NZ):
            for c in range(NC):
                far = outer(z, c, NZ)
                rows = []
                for zs in ((z, inner(z, c, NZ)), (far, inner(far, c, NZ))):
                    rows += [2 * (xx * NZ + zz) + c for xx in range(NX) for zz in zs]
                table[x * NZ + z, c] = rows
    return table


def block_table():
    table = np.zeros((16, 8), np.int32)
    for y in range(NY):
        for c in range(NC):
            v = (y - c) % NY
            k, s = v // 2, v % 2
            far = (k + 2) % 4
            mid = (k + 1 - 2 * s) % 4
            near = (k - 1 + 2 * s) % 4
            order = [2 * far + s, 2 * far + 1 - s]
            order += [2 * mid + 1 - s, 2 * mid + s]
            order += [2 * near + s, 2 * near + 1 - s]
            order += [2 * k + 1 - s, 2 * k + s]
            table[y * NC + c] = [2 * ((b + c) % NY) + c for b in order]
    return table


SMEM = pl.BlockSpec(memory_space=pltpu.SMEM)
VMEM = pl.BlockSpec(memory_space=pltpu.VMEM)
HBM = pl.BlockSpec(memory_space=pltpu.HBM)


def grant(mib):
    return pltpu.CompilerParams(vmem_limit_bytes=mib * 2**20)


def prepare_kernel(k_ref, v_ref, mask_hbm, out_ref, mask_ref, sems):
    counted = pltpu.make_async_copy(mask_hbm, mask_ref, sems.at[2])
    counted.start()
    tensor = lax.axis_index("tensor")
    rows = pl.ds(pl.multiple_of(lax.rem(tensor, NC) * SPAN, SPAN), SPAN)
    cols = pl.ds(pl.multiple_of(lax.div(tensor, NC) * HD, HD), HD)
    copies = []
    for i, ref in enumerate((k_ref, v_ref)):
        into = out_ref.at[pl.ds(0, SPAN), pl.ds(i * HD, HD)]
        copies.append(pltpu.make_async_copy(ref.at[0, rows, cols], into, sems.at[i]))
        copies[-1].start()
    counted.wait()
    total = jnp.sum(mask_ref[...].astype(jnp.float32), axis=1, keepdims=True)
    out_ref[SPAN:, :] = jnp.broadcast_to(total, (TALLY, 2 * HD)).astype(jnp.bfloat16)
    for copy in copies:
        copy.wait()


def prepare(keys, values, loss_mask):
    return pl.pallas_call(
        prepare_kernel,
        out_shape=jax.ShapeDtypeStruct((BLOCK, 2 * HD), jnp.bfloat16),
        in_specs=[HBM] * 3,
        out_specs=VMEM,
        scratch_shapes=[pltpu.VMEM(loss_mask.shape, loss_mask.dtype), pltpu.SemaphoreType.DMA((3,))],
        compiler_params=grant(2),
        name="prepare",
    )(keys, values, loss_mask)


def pack_kernel(order, w_ref, out_ref, sems):
    other = (lax.axis_index("tensor") ^ 1) * 8
    copies = []
    for g in range(8):
        at = pl.multiple_of(order[other + g] * COLS, COLS)
        copies.append(pltpu.make_async_copy(w_ref.at[:, pl.ds(at, COLS)], out_ref.at[g], sems.at[g]))
        copies[-1].start()
    for copy in copies:
        copy.wait()


def pack(order, w):
    return pl.pallas_call(
        pack_kernel,
        out_shape=jax.ShapeDtypeStruct((8, w.shape[0], COLS), w.dtype),
        in_specs=[SMEM, HBM],
        out_specs=HBM,
        scratch_shapes=[pltpu.SemaphoreType.DMA((8,))],
        compiler_params=grant(2),
        name="pack",
    )(order, w)


def attention_kernel(
    slots, spans, seg_ref, q_ref, q_other_ref, a_ref, b_ref, out_ref, tally_ref, kv, q8, items, lo_ref, m_ref, l_ref, acc
):
    f32 = jnp.float32
    context = lax.axis_index("context")
    core = lax.rem(lax.axis_index("tensor"), NC)
    heads = 2 * q_ref.shape[1] // HD
    half = heads // 2
    width = heads * SPAN
    tally = jnp.zeros((TALLY, HD), f32)
    for which, ref in enumerate((a_ref, b_ref)):
        for i in range(8):
            kv[which * 8 + i] = ref[i * BLOCK : i * BLOCK + SPAN, :]
            tally += ref[i * BLOCK + SPAN : (i + 1) * BLOCK, :HD].astype(f32)
    tally_ref[...] = tally
    seg = seg_ref[...]
    starts = [jnp.sum((seg < d).astype(f32), keepdims=True) for d in range(1, 8)]
    base = (context * NC + core) * 16
    count = jnp.int32(0)
    for i in range(2):
        for h in range(heads):
            ref = q_ref if h < half else q_other_ref
            q8[i, h * SPAN : (h + 1) * SPAN, :] = ref[i * SPAN : (i + 1) * SPAN, h % half * HD : (h % half + 1) * HD]
        q_seg = seg_ref[pl.ds(2 * context + i, 1), :]
        lo = jnp.zeros((1, SPAN), f32)
        for d in range(1, 8):
            lo = jnp.where(q_seg == d, starts[d - 1], lo)
        lo_ref[i] = lo
        first = jnp.min(lo).astype(jnp.int32)
        q_pos = spans[2 * context + i]
        m_ref[i] = jnp.full((1, width), LOW, f32)
        l_ref[i] = jnp.zeros((1, width), f32)
        acc[i] = jnp.zeros((HD, width), f32)
        for b in range(16):
            pos = spans[slots[base + b]]
            items[count] = i * 16 + b
            seen = (pos <= q_pos) & ((pos + 1) * SPAN > first)
            count = count + seen.astype(jnp.int32)

    def step(j, carry):
        item = items[j]
        i, b = lax.shift_right_logical(item, 4), item & 15
        pos = lax.broadcasted_iota(jnp.int32, (SPAN, SPAN), 0) + spans[slots[base + b]] * SPAN
        hi = lax.broadcasted_iota(jnp.int32, (SPAN, SPAN), 1) + spans[2 * context + i] * SPAN
        bias = jnp.where((pos.astype(f32) >= lo_ref[i]) & (pos <= hi), 0.0, LOW)
        s = lax.dot_general(kv[b, :, :HD], q8[i], (((1,), (1,)), ((), ())), preferred_element_type=f32)
        s = s * (HD ** (-0.5) * LOG2E) + jnp.concatenate([bias] * heads, axis=1)
        old = m_ref[i]
        new = jnp.maximum(old, jnp.max(s, axis=0, keepdims=True))
        alpha = jnp.exp2(old - new)
        p = jnp.exp2(s - new)
        m_ref[i] = new
        l_ref[i] = l_ref[i] * alpha + jnp.sum(p, axis=0, keepdims=True)
        add = lax.dot_general(
            kv[b, :, HD:], p.astype(jnp.bfloat16), (((0,), (0,)), ((), ())), preferred_element_type=f32
        )
        acc[i] = acc[i] * alpha + add
        return carry

    lax.fori_loop(0, count, step, 0)
    row = lax.broadcasted_iota(jnp.int32, (TALLY, width), 0)
    for i in range(2):
        cols = slice(i * width, (i + 1) * width)
        total = l_ref[i]
        total = jnp.where(total > 0, total, 1.0)
        out_ref[:SPAN, cols] = (acc[i] / total).astype(jnp.bfloat16)
        log = m_ref[i] + jnp.log(total) * LOG2E
        high = log.astype(jnp.bfloat16).astype(f32)
        mid = (log - high).astype(jnp.bfloat16).astype(f32)
        tail = log - high - mid
        parts = jnp.where(row == 0, high, jnp.where(row == 1, mid, jnp.where(row == 2, tail, 0.0)))
        out_ref[SPAN:, cols] = parts.astype(jnp.bfloat16)


def attention(slots, spans, seg, q, q_other, a, b):
    heads = 2 * q.shape[1] // HD
    width = heads * SPAN
    return pl.pallas_call(
        attention_kernel,
        out_shape=(
            jax.ShapeDtypeStruct((BLOCK, 2 * width), jnp.bfloat16),
            jax.ShapeDtypeStruct((TALLY, HD), jnp.float32),
        ),
        in_specs=[SMEM, SMEM] + [VMEM] * 5,
        out_specs=(VMEM, VMEM),
        scratch_shapes=[
            pltpu.VMEM((16, SPAN, 2 * HD), jnp.bfloat16),
            pltpu.VMEM((2, width, HD), jnp.bfloat16),
            pltpu.SMEM((33,), jnp.int32),
            pltpu.VMEM((2, 1, SPAN), jnp.float32),
            pltpu.VMEM((2, 1, width), jnp.float32),
            pltpu.VMEM((2, 1, width), jnp.float32),
            pltpu.VMEM((2, HD, width), jnp.float32),
        ],
        compiler_params=grant(12),
        name="attend",
    )(slots, spans, seg, q, q_other, a, b)


def multiply(order, first, heads_ref, w_ref, other_ref, out_ref):
    depth = w_ref.shape[0]
    mine = lax.axis_index("tensor") * 8
    for g in range(out_ref.shape[0]):
        at = pl.multiple_of(order[mine + first + g] * COLS, COLS)
        total = jnp.dot(heads_ref[:, :depth], w_ref[:, pl.ds(at, COLS)], preferred_element_type=jnp.float32)
        total += jnp.dot(heads_ref[:, depth:], other_ref[first + g], preferred_element_type=jnp.float32)
        out_ref[g] = total.astype(jnp.bfloat16)


def join_kernel(order, mine_ref, theirs_ref, w_ref, other_ref, heads_ref, out_ref):
    f32 = jnp.float32
    width = mine_ref.shape[1] // 2
    heads = width // SPAN

    def log(ref, at):
        rows = ref[SPAN:, at : at + SPAN].astype(f32)
        return rows[0:1] + rows[1:2] + rows[2:3]

    for i in range(2):
        for h in range(heads):
            a = i * width + h * SPAN
            b = i * width + (h + heads // 2) % heads * SPAN
            log_a, log_b = log(mine_ref, a), log(theirs_ref, b)
            top = jnp.maximum(log_a, log_b)
            part_a, part_b = jnp.exp2(log_a - top), jnp.exp2(log_b - top)
            total = part_a + part_b
            joined = mine_ref[:SPAN, a : a + SPAN].astype(f32) * (part_a / total)
            joined += theirs_ref[:SPAN, b : b + SPAN].astype(f32) * (part_b / total)
            heads_ref[i * SPAN : (i + 1) * SPAN, h * HD : (h + 1) * HD] = joined.T.astype(jnp.bfloat16)
    multiply(order, 0, heads_ref, w_ref, other_ref, out_ref)


def join(order, mine, theirs, w, other):
    rows, depth = 2 * SPAN, 2 * w.shape[0]
    return pl.pallas_call(
        join_kernel,
        out_shape=(
            jax.ShapeDtypeStruct((rows, depth), jnp.bfloat16),
            jax.ShapeDtypeStruct((2, rows, COLS), jnp.bfloat16),
        ),
        in_specs=[SMEM] + [VMEM] * 4,
        out_specs=(VMEM, VMEM),
        compiler_params=grant(20),
        name="join",
    )(order, mine, theirs, w, other)


def project_kernel(order, heads_ref, w_ref, other_ref, out_ref):
    multiply(order, 2, heads_ref, w_ref, other_ref, out_ref)


def project(order, heads, w, other):
    rows = heads.shape[0]
    return pl.pallas_call(
        project_kernel,
        out_shape=jax.ShapeDtypeStruct((6, rows, COLS), jnp.bfloat16),
        in_specs=[SMEM] + [VMEM] * 3,
        out_specs=VMEM,
        compiler_params=grant(20),
        name="project",
    )(order, heads, w, other)


def add(a, b):
    return (a.astype(jnp.float32) + b.astype(jnp.float32)).astype(jnp.bfloat16)


def per_device(queries, keys, values, out_weight, segment_ids, loss_mask, span_order):
    both = ("context", "tensor")
    f32 = jnp.float32
    cat = lambda *a: jnp.concatenate(a, axis=0)
    order = jnp.asarray(block_table().reshape(-1))
    slots = jnp.asarray(slot_table().reshape(-1))
    along_x = [[x * NZ + z for x in range(NX)] for z in range(NZ)]
    gather = lambda a: lax.all_gather(a, "context", axis=0, tiled=True, axis_index_groups=along_x)

    in_hbm = lambda a: pltpu.with_memory_space_constraint(a, pltpu.HBM)

    kv1 = prepare(in_hbm(keys), in_hbm(values), in_hbm(loss_mask))
    r1 = lax.ppermute(kv1, both, perm_context("z", inner))
    q_other = lax.ppermute(queries[0], "tensor", SWAP)
    packed = pack(order, in_hbm(out_weight))
    weight_other = lax.ppermute(packed, "tensor", SWAP)
    kv2 = cat(kv1, r1)
    r2 = lax.ppermute(kv2, both, perm_context("z", outer))
    near = gather(kv2)
    far = gather(r2)
    mine, tally = attention(slots, span_order, segment_ids.reshape(32, SPAN), queries[0], q_other, near, far)
    theirs = lax.ppermute(mine, "tensor", SWAP)

    inward, outward = perm_tensor(inner), perm_tensor(outer)
    heads, far = join(order, mine, theirs, out_weight, weight_other)
    far = lax.ppermute(far, "tensor", outward)
    rest = project(order, heads, out_weight, weight_other)
    around = [(d * 16 + t, (d + 1 + t % 2) % 3 * 16 + t) for d in range(3) for t in range(16)]
    one = lax.ppermute(tally, ("dp", "tensor"), around)
    two = lax.ppermute(one, "tensor", SWAP)
    mid = lax.ppermute(add(rest[0:2], far), "tensor", inward)
    near = lax.ppermute(add(rest[2:4], mid), "tensor", outward)
    last = lax.ppermute(add(rest[4], near[0]), "tensor", inward)
    count = (tally + one + two)[0, 0]
    scale_all = lax.axis_size("dp") * lax.axis_size("context") * queries.shape[1]
    weight = loss_mask[0].astype(f32) * scale_all / count
    summed = rest[5].astype(f32) + near[1].astype(f32) + last.astype(f32)
    return (summed * weight[:, None]).astype(jnp.bfloat16)[None]


def solution(mesh):
    in_specs = (
        P("dp", "context", "tensor"),
        P("dp", "context", None),
        P("dp", "context", None),
        P("tensor", None),
        P("dp", None),
        P("dp", "context"),
        P(),
    )
    out_specs = P("dp", "context", "tensor")
    return jax.shard_map(
        per_device, mesh=mesh, in_specs=in_specs, out_specs=out_specs, check_vma=False
    )
```

```python
import jax
import jax.numpy as jnp
import numpy as np
from jax import lax
from jax.experimental import pallas as pl
from jax.experimental.pallas import tpu as pltpu
from jax.sharding import PartitionSpec as P


HD = 128
SPAN = 128
TALLY = 8
BLOCK = SPAN + TALLY
COLS = 512
LOG2E = 1.4426950408889634
LOW = -1e30


NX, NZ, NY, NC = 4, 4, 8, 2


def inner(i, c, n):
    return ((((i - c) % n) ^ 1) + c) % n


def outer(i, c, n):
    v = (i - c) % n
    return (v + (1 if v % 2 else -1) + c) % n


def perm_context(axis, partner):
    out = []
    for x in range(NX):
        for z in range(NZ):
            for y in range(NY):
                for c in range(NC):
                    px = partner(x, c, NX) if axis == "x" else x
                    pz = partner(z, c, NZ) if axis == "z" else z
                    tensor = y * NC + c
                    out.append(((x * NZ + z) * 16 + tensor, (px * NZ + pz) * 16 + tensor))
    return out


def perm_tensor(partner):
    return [
        (y * NC + c, partner(y, c, NY) * NC + c) for y in range(NY) for c in range(NC)
    ]


SWAP = [(t, t ^ 1) for t in range(16)]


def slot_table():
    table = np.zeros((16, NC, 16), np.int32)
    for x in range(NX):
        for z in range(NZ):
            for c in range(NC):
                far = outer(z, c, NZ)
                rows = []
                for zs in ((z,), (inner(z, c, NZ), far, inner(far, c, NZ))):
                    rows += [2 * (xx * NZ + zz) + c for xx in range(NX) for zz in zs]
                table[x * NZ + z, c] = rows
    return table


def block_table():
    table = np.zeros((16, 8), np.int32)
    for y in range(NY):
        for c in range(NC):
            v = (y - c) % NY
            k, s = v // 2, v % 2
            far = (k + 2) % 4
            mid = (k + 1 - 2 * s) % 4
            near = (k - 1 + 2 * s) % 4
            order = [2 * far + s, 2 * far + 1 - s]
            order += [2 * mid + 1 - s, 2 * mid + s]
            order += [2 * near + s, 2 * near + 1 - s]
            order += [2 * k + 1 - s, 2 * k + s]
            table[y * NC + c] = [2 * ((b + c) % NY) + c for b in order]
    return table


SMEM = pl.BlockSpec(memory_space=pltpu.SMEM)
VMEM = pl.BlockSpec(memory_space=pltpu.VMEM)
HBM = pl.BlockSpec(memory_space=pltpu.HBM)


def grant(mib):
    return pltpu.CompilerParams(vmem_limit_bytes=mib * 2**20)


def prepare_kernel(k_ref, v_ref, mask_hbm, out_ref, mask_ref, sems):
    counted = pltpu.make_async_copy(mask_hbm, mask_ref, sems.at[2])
    counted.start()
    tensor = lax.axis_index("tensor")
    rows = pl.ds(pl.multiple_of(lax.rem(tensor, NC) * SPAN, SPAN), SPAN)
    cols = pl.ds(pl.multiple_of(lax.div(tensor, NC) * HD, HD), HD)
    copies = []
    for i, ref in enumerate((k_ref, v_ref)):
        into = out_ref.at[pl.ds(0, SPAN), pl.ds(i * HD, HD)]
        copies.append(pltpu.make_async_copy(ref.at[0, rows, cols], into, sems.at[i]))
        copies[-1].start()
    counted.wait()
    total = jnp.sum(mask_ref[...].astype(jnp.float32), axis=1, keepdims=True)
    out_ref[SPAN:, :] = jnp.broadcast_to(total, (TALLY, 2 * HD)).astype(jnp.bfloat16)
    for copy in copies:
        copy.wait()


def prepare(keys, values, loss_mask):
    return pl.pallas_call(
        prepare_kernel,
        out_shape=jax.ShapeDtypeStruct((BLOCK, 2 * HD), jnp.bfloat16),
        in_specs=[HBM] * 3,
        out_specs=VMEM,
        scratch_shapes=[pltpu.VMEM(loss_mask.shape, loss_mask.dtype), pltpu.SemaphoreType.DMA((3,))],
        compiler_params=grant(2),
        name="prepare",
    )(keys, values, loss_mask)


def pack_kernel(order, w_ref, out_ref, sems):
    other = (lax.axis_index("tensor") ^ 1) * 8
    copies = []
    for g in range(8):
        at = pl.multiple_of(order[other + g] * COLS, COLS)
        copies.append(pltpu.make_async_copy(w_ref.at[:, pl.ds(at, COLS)], out_ref.at[g], sems.at[g]))
        copies[-1].start()
    for copy in copies:
        copy.wait()


def pack(order, w):
    return pl.pallas_call(
        pack_kernel,
        out_shape=jax.ShapeDtypeStruct((8, w.shape[0], COLS), w.dtype),
        in_specs=[SMEM, HBM],
        out_specs=HBM,
        scratch_shapes=[pltpu.SemaphoreType.DMA((8,))],
        compiler_params=grant(2),
        name="pack",
    )(order, w)


def attention_kernel(
    slots, spans, seg_ref, q_ref, q_other_ref, a_ref, b_ref, out_ref, tally_ref, kv, q8, items, lo_ref, m_ref, l_ref, acc
):
    f32 = jnp.float32
    context = lax.axis_index("context")
    core = lax.rem(lax.axis_index("tensor"), NC)
    heads = 2 * q_ref.shape[1] // HD
    half = heads // 2
    width = heads * SPAN
    tally = jnp.zeros((TALLY, HD), f32)
    at = 0
    for ref in (a_ref, b_ref):
        for i in range(ref.shape[0] // BLOCK):
            kv[at] = ref[i * BLOCK : i * BLOCK + SPAN, :]
            tally += ref[i * BLOCK + SPAN : (i + 1) * BLOCK, :HD].astype(f32)
            at += 1
    tally_ref[...] = tally
    seg = seg_ref[...]
    starts = [jnp.sum((seg < d).astype(f32), keepdims=True) for d in range(1, 8)]
    base = (context * NC + core) * 16
    count = jnp.int32(0)
    for i in range(2):
        for h in range(heads):
            ref = q_ref if h < half else q_other_ref
            q8[i, h * SPAN : (h + 1) * SPAN, :] = ref[i * SPAN : (i + 1) * SPAN, h % half * HD : (h % half + 1) * HD]
        q_seg = seg_ref[pl.ds(2 * context + i, 1), :]
        lo = jnp.zeros((1, SPAN), f32)
        for d in range(1, 8):
            lo = jnp.where(q_seg == d, starts[d - 1], lo)
        lo_ref[i] = lo
        first = jnp.min(lo).astype(jnp.int32)
        q_pos = spans[2 * context + i]
        m_ref[i] = jnp.full((1, width), LOW, f32)
        l_ref[i] = jnp.zeros((1, width), f32)
        acc[i] = jnp.zeros((HD, width), f32)
        for b in range(16):
            pos = spans[slots[base + b]]
            items[count] = i * 16 + b
            seen = (pos <= q_pos) & ((pos + 1) * SPAN > first)
            count = count + seen.astype(jnp.int32)

    def step(j, carry):
        item = items[j]
        i, b = lax.shift_right_logical(item, 4), item & 15
        pos = lax.broadcasted_iota(jnp.int32, (SPAN, SPAN), 0) + spans[slots[base + b]] * SPAN
        hi = lax.broadcasted_iota(jnp.int32, (SPAN, SPAN), 1) + spans[2 * context + i] * SPAN
        bias = jnp.where((pos.astype(f32) >= lo_ref[i]) & (pos <= hi), 0.0, LOW)
        s = lax.dot_general(kv[b, :, :HD], q8[i], (((1,), (1,)), ((), ())), preferred_element_type=f32)
        s = s * (HD ** (-0.5) * LOG2E) + jnp.concatenate([bias] * heads, axis=1)
        old = m_ref[i]
        new = jnp.maximum(old, jnp.max(s, axis=0, keepdims=True))
        alpha = jnp.exp2(old - new)
        p = jnp.exp2(s - new)
        m_ref[i] = new
        l_ref[i] = l_ref[i] * alpha + jnp.sum(p, axis=0, keepdims=True)
        add = lax.dot_general(
            kv[b, :, HD:], p.astype(jnp.bfloat16), (((0,), (0,)), ((), ())), preferred_element_type=f32
        )
        acc[i] = acc[i] * alpha + add
        return carry

    lax.fori_loop(0, count, step, 0)
    row = lax.broadcasted_iota(jnp.int32, (TALLY, width), 0)
    for i in range(2):
        cols = slice(i * width, (i + 1) * width)
        total = l_ref[i]
        total = jnp.where(total > 0, total, 1.0)
        out_ref[:SPAN, cols] = (acc[i] / total).astype(jnp.bfloat16)
        log = m_ref[i] + jnp.log(total) * LOG2E
        high = log.astype(jnp.bfloat16).astype(f32)
        mid = (log - high).astype(jnp.bfloat16).astype(f32)
        tail = log - high - mid
        parts = jnp.where(row == 0, high, jnp.where(row == 1, mid, jnp.where(row == 2, tail, 0.0)))
        out_ref[SPAN:, cols] = parts.astype(jnp.bfloat16)


def attention(slots, spans, seg, q, q_other, a, b):
    heads = 2 * q.shape[1] // HD
    width = heads * SPAN
    return pl.pallas_call(
        attention_kernel,
        out_shape=(
            jax.ShapeDtypeStruct((BLOCK, 2 * width), jnp.bfloat16),
            jax.ShapeDtypeStruct((TALLY, HD), jnp.float32),
        ),
        in_specs=[SMEM, SMEM] + [VMEM] * 5,
        out_specs=(VMEM, VMEM),
        scratch_shapes=[
            pltpu.VMEM((16, SPAN, 2 * HD), jnp.bfloat16),
            pltpu.VMEM((2, width, HD), jnp.bfloat16),
            pltpu.SMEM((33,), jnp.int32),
            pltpu.VMEM((2, 1, SPAN), jnp.float32),
            pltpu.VMEM((2, 1, width), jnp.float32),
            pltpu.VMEM((2, 1, width), jnp.float32),
            pltpu.VMEM((2, HD, width), jnp.float32),
        ],
        compiler_params=grant(12),
        name="attend",
    )(slots, spans, seg, q, q_other, a, b)


def multiply(order, first, heads_ref, w_ref, other_ref, out_ref):
    depth = w_ref.shape[0]
    mine = lax.axis_index("tensor") * 8
    for g in range(out_ref.shape[0]):
        at = pl.multiple_of(order[mine + first + g] * COLS, COLS)
        total = jnp.dot(heads_ref[:, :depth], w_ref[:, pl.ds(at, COLS)], preferred_element_type=jnp.float32)
        total += jnp.dot(heads_ref[:, depth:], other_ref[first + g], preferred_element_type=jnp.float32)
        out_ref[g] = total.astype(jnp.bfloat16)


def join_kernel(order, mine_ref, theirs_ref, w_ref, other_ref, heads_ref, out_ref):
    f32 = jnp.float32
    width = mine_ref.shape[1] // 2
    heads = width // SPAN

    def log(ref, at):
        rows = ref[SPAN:, at : at + SPAN].astype(f32)
        return rows[0:1] + rows[1:2] + rows[2:3]

    for i in range(2):
        for h in range(heads):
            a = i * width + h * SPAN
            b = i * width + (h + heads // 2) % heads * SPAN
            log_a, log_b = log(mine_ref, a), log(theirs_ref, b)
            top = jnp.maximum(log_a, log_b)
            part_a, part_b = jnp.exp2(log_a - top), jnp.exp2(log_b - top)
            total = part_a + part_b
            joined = mine_ref[:SPAN, a : a + SPAN].astype(f32) * (part_a / total)
            joined += theirs_ref[:SPAN, b : b + SPAN].astype(f32) * (part_b / total)
            heads_ref[i * SPAN : (i + 1) * SPAN, h * HD : (h + 1) * HD] = joined.T.astype(jnp.bfloat16)
    multiply(order, 0, heads_ref, w_ref, other_ref, out_ref)


def join(order, mine, theirs, w, other):
    rows, depth = 2 * SPAN, 2 * w.shape[0]
    return pl.pallas_call(
        join_kernel,
        out_shape=(
            jax.ShapeDtypeStruct((rows, depth), jnp.bfloat16),
            jax.ShapeDtypeStruct((2, rows, COLS), jnp.bfloat16),
        ),
        in_specs=[SMEM] + [VMEM] * 4,
        out_specs=(VMEM, VMEM),
        compiler_params=grant(20),
        name="join",
    )(order, mine, theirs, w, other)


def project_kernel(order, heads_ref, w_ref, other_ref, out_ref):
    multiply(order, 2, heads_ref, w_ref, other_ref, out_ref)


def project(order, heads, w, other):
    rows = heads.shape[0]
    return pl.pallas_call(
        project_kernel,
        out_shape=jax.ShapeDtypeStruct((6, rows, COLS), jnp.bfloat16),
        in_specs=[SMEM] + [VMEM] * 3,
        out_specs=VMEM,
        compiler_params=grant(20),
        name="project",
    )(order, heads, w, other)


def add(a, b):
    return (a.astype(jnp.float32) + b.astype(jnp.float32)).astype(jnp.bfloat16)


def per_device(queries, keys, values, out_weight, segment_ids, loss_mask, span_order):
    both = ("context", "tensor")
    f32 = jnp.float32
    cat = lambda *a: jnp.concatenate(a, axis=0)
    order = jnp.asarray(block_table().reshape(-1))
    slots = jnp.asarray(slot_table().reshape(-1))
    along_x = [[x * NZ + z for x in range(NX)] for z in range(NZ)]
    gather = lambda a: lax.all_gather(a, "context", axis=0, tiled=True, axis_index_groups=along_x)

    in_hbm = lambda a: pltpu.with_memory_space_constraint(a, pltpu.HBM)

    kv1 = prepare(in_hbm(keys), in_hbm(values), in_hbm(loss_mask))
    r1 = lax.ppermute(kv1, both, perm_context("z", inner))
    near = gather(kv1)
    r2 = lax.ppermute(cat(kv1, r1), both, perm_context("z", outer))
    q_other = lax.ppermute(queries[0], "tensor", SWAP)
    packed = pack(order, in_hbm(out_weight))
    weight_other = lax.ppermute(packed, "tensor", SWAP)
    far = gather(cat(r1, r2))
    mine, tally = attention(slots, span_order, segment_ids.reshape(32, SPAN), queries[0], q_other, near, far)
    theirs = lax.ppermute(mine, "tensor", SWAP)

    inward, outward = perm_tensor(inner), perm_tensor(outer)
    heads, far = join(order, mine, theirs, out_weight, weight_other)
    far = lax.ppermute(far, "tensor", outward)
    rest = project(order, heads, out_weight, weight_other)
    around = [(d * 16 + t, (d + 1 + t % 2) % 3 * 16 + t) for d in range(3) for t in range(16)]
    one = lax.ppermute(tally, ("dp", "tensor"), around)
    two = lax.ppermute(one, "tensor", SWAP)
    mid = lax.ppermute(add(rest[0:2], far), "tensor", inward)
    near = lax.ppermute(add(rest[2:4], mid), "tensor", outward)
    last = lax.ppermute(add(rest[4], near[0]), "tensor", inward)
    count = (tally + one + two)[0, 0]
    scale_all = lax.axis_size("dp") * lax.axis_size("context") * queries.shape[1]
    weight = loss_mask[0].astype(f32) * scale_all / count
    summed = rest[5].astype(f32) + near[1].astype(f32) + last.astype(f32)
    return (summed * weight[:, None]).astype(jnp.bfloat16)[None]


def solution(mesh):
    in_specs = (
        P("dp", "context", "tensor"),
        P("dp", "context", None),
        P("dp", "context", None),
        P("tensor", None),
        P("dp", None),
        P("dp", "context"),
        P(),
    )
    out_specs = P("dp", "context", "tensor")
    return jax.shard_map(
        per_device, mesh=mesh, in_specs=in_specs, out_specs=out_specs, check_vma=False
    )
```

```python
import jax
import jax.numpy as jnp
from jax import lax
from jax.experimental import pallas as pl
from jax.experimental.pallas import tpu as pltpu
from jax.sharding import PartitionSpec as P


HD = 128
SPAN = 128
TALLY = 8
BLOCK = SPAN + TALLY
COLS = 512
LOG2E = 1.4426950408889634
LOW = -1e30


NX, NZ, NY, NC = 4, 4, 8, 2


def inner(i, c, n):
    return ((((i - c) & (n - 1)) ^ 1) + c) & (n - 1)


def outer(i, c, n):
    v = (i - c) & (n - 1)
    return (v + 2 * (v & 1) - 1 + c) & (n - 1)


def perm_context(axis, partner):
    out = []
    for x in range(NX):
        for z in range(NZ):
            for y in range(NY):
                for c in range(NC):
                    px = partner(x, c, NX) if axis == "x" else x
                    pz = partner(z, c, NZ) if axis == "z" else z
                    tensor = y * NC + c
                    out.append(((x * NZ + z) * 16 + tensor, (px * NZ + pz) * 16 + tensor))
    return out


def perm_tensor(partner):
    return [
        (y * NC + c, partner(y, c, NY) * NC + c) for y in range(NY) for c in range(NC)
    ]


SWAP = [(t, t ^ 1) for t in range(16)]


def gathered_slot(context, core, i):
    z = context & (NZ - 1)
    far = outer(z, core, NZ)
    if i < NX:
        return 2 * (i * NZ + z) + core
    x, which = divmod(i - NX, NZ - 1)
    zs = (inner(z, core, NZ), far, inner(far, core, NZ))
    return 2 * (x * NZ + zs[which]) + core


def column_blocks(tensor):
    y, core = tensor >> 1, tensor & 1
    v = (y - core) & (NY - 1)
    k, s = v >> 1, v & 1
    far, mid, near = (k + 2) & 3, (k + 1 - 2 * s) & 3, (k - 1 + 2 * s) & 3
    order = (2 * far + s, 2 * far + 1 - s, 2 * mid + 1 - s, 2 * mid + s)
    order += (2 * near + s, 2 * near + 1 - s, 2 * k + 1 - s, 2 * k + s)
    return [2 * ((b + core) & (NY - 1)) + core for b in order]


SMEM = pl.BlockSpec(memory_space=pltpu.SMEM)
VMEM = pl.BlockSpec(memory_space=pltpu.VMEM)
HBM = pl.BlockSpec(memory_space=pltpu.HBM)


def grant(mib):
    return pltpu.CompilerParams(vmem_limit_bytes=mib * 2**20)


def prepare_kernel(k_ref, v_ref, mask_hbm, out_ref, mask_ref, sems):
    counted = pltpu.make_async_copy(mask_hbm, mask_ref, sems.at[2])
    counted.start()
    tensor = lax.axis_index("tensor")
    rows = pl.ds(pl.multiple_of(lax.rem(tensor, NC) * SPAN, SPAN), SPAN)
    cols = pl.ds(pl.multiple_of(lax.div(tensor, NC) * HD, HD), HD)
    copies = []
    for i, ref in enumerate((k_ref, v_ref)):
        into = out_ref.at[pl.ds(0, SPAN), pl.ds(i * HD, HD)]
        copies.append(pltpu.make_async_copy(ref.at[0, rows, cols], into, sems.at[i]))
        copies[-1].start()
    counted.wait()
    total = jnp.sum(mask_ref[...].astype(jnp.float32), axis=1, keepdims=True)
    out_ref[SPAN:, :] = jnp.broadcast_to(total, (TALLY, 2 * HD)).astype(jnp.bfloat16)
    for copy in copies:
        copy.wait()


def prepare(keys, values, loss_mask):
    return pl.pallas_call(
        prepare_kernel,
        out_shape=jax.ShapeDtypeStruct((BLOCK, 2 * HD), jnp.bfloat16),
        in_specs=[HBM] * 3,
        out_specs=VMEM,
        scratch_shapes=[pltpu.VMEM(loss_mask.shape, loss_mask.dtype), pltpu.SemaphoreType.DMA((3,))],
        compiler_params=grant(2),
        name="prepare",
    )(keys, values, loss_mask)


def pack_kernel(w_ref, out_ref, sems):
    copies = []
    for g, block in enumerate(column_blocks(lax.axis_index("tensor") ^ 1)):
        at = pl.multiple_of(block * COLS, COLS)
        copies.append(pltpu.make_async_copy(w_ref.at[:, pl.ds(at, COLS)], out_ref.at[g], sems.at[g]))
        copies[-1].start()
    for copy in copies:
        copy.wait()


def pack(w):
    return pl.pallas_call(
        pack_kernel,
        out_shape=jax.ShapeDtypeStruct((8, w.shape[0], COLS), w.dtype),
        in_specs=[HBM],
        out_specs=HBM,
        scratch_shapes=[pltpu.SemaphoreType.DMA((8,))],
        compiler_params=grant(2),
        name="pack",
    )(w)


def attention_kernel(
    spans, seg_ref, q_ref, q_other_ref, a_ref, b_ref, out_ref, tally_ref, kv, q8, places, items, lo_ref, m_ref, l_ref, acc
):
    f32 = jnp.float32
    context = lax.axis_index("context")
    core = lax.rem(lax.axis_index("tensor"), NC)
    heads = 2 * q_ref.shape[1] // HD
    half = heads // 2
    width = heads * SPAN
    tally = jnp.zeros((TALLY, HD), f32)
    at = 0
    for ref in (a_ref, b_ref):
        for i in range(ref.shape[0] // BLOCK):
            kv[at] = ref[i * BLOCK : i * BLOCK + SPAN, :]
            tally += ref[i * BLOCK + SPAN : (i + 1) * BLOCK, :HD].astype(f32)
            at += 1
    tally_ref[...] = tally
    seg = seg_ref[...]
    starts = [jnp.sum((seg < d).astype(f32), keepdims=True) for d in range(1, 8)]
    count = jnp.int32(0)
    for b in range(16):
        places[b] = spans[gathered_slot(context, core, b)]
    for i in range(2):
        for h in range(heads):
            ref = q_ref if h < half else q_other_ref
            q8[i, h * SPAN : (h + 1) * SPAN, :] = ref[i * SPAN : (i + 1) * SPAN, h % half * HD : (h % half + 1) * HD]
        q_seg = seg_ref[pl.ds(2 * context + i, 1), :]
        lo = jnp.zeros((1, SPAN), f32)
        for d in range(1, 8):
            lo = jnp.where(q_seg == d, starts[d - 1], lo)
        lo_ref[i] = lo
        first = jnp.min(lo).astype(jnp.int32)
        q_pos = spans[2 * context + i]
        m_ref[i] = jnp.full((1, width), LOW, f32)
        l_ref[i] = jnp.zeros((1, width), f32)
        acc[i] = jnp.zeros((HD, width), f32)
        for b in range(16):
            pos = places[b]
            items[count] = i * 16 + b
            seen = (pos <= q_pos) & ((pos + 1) * SPAN > first)
            count = count + seen.astype(jnp.int32)

    def step(j, carry):
        item = items[j]
        i, b = lax.shift_right_logical(item, 4), item & 15
        pos = lax.broadcasted_iota(jnp.int32, (SPAN, SPAN), 0) + places[b] * SPAN
        hi = lax.broadcasted_iota(jnp.int32, (SPAN, SPAN), 1) + spans[2 * context + i] * SPAN
        bias = jnp.where((pos.astype(f32) >= lo_ref[i]) & (pos <= hi), 0.0, LOW)
        s = lax.dot_general(kv[b, :, :HD], q8[i], (((1,), (1,)), ((), ())), preferred_element_type=f32)
        s = s * (HD ** (-0.5) * LOG2E) + jnp.concatenate([bias] * heads, axis=1)
        old = m_ref[i]
        new = jnp.maximum(old, jnp.max(s, axis=0, keepdims=True))
        alpha = jnp.exp2(old - new)
        p = jnp.exp2(s - new)
        m_ref[i] = new
        l_ref[i] = l_ref[i] * alpha + jnp.sum(p, axis=0, keepdims=True)
        add = lax.dot_general(
            kv[b, :, HD:], p.astype(jnp.bfloat16), (((0,), (0,)), ((), ())), preferred_element_type=f32
        )
        acc[i] = acc[i] * alpha + add
        return carry

    lax.fori_loop(0, count, step, 0)
    row = lax.broadcasted_iota(jnp.int32, (TALLY, width), 0)
    for i in range(2):
        cols = slice(i * width, (i + 1) * width)
        total = l_ref[i]
        total = jnp.where(total > 0, total, 1.0)
        out_ref[:SPAN, cols] = (acc[i] / total).astype(jnp.bfloat16)
        log = m_ref[i] + jnp.log(total) * LOG2E
        high = log.astype(jnp.bfloat16).astype(f32)
        mid = (log - high).astype(jnp.bfloat16).astype(f32)
        tail = log - high - mid
        parts = jnp.where(row == 0, high, jnp.where(row == 1, mid, jnp.where(row == 2, tail, 0.0)))
        out_ref[SPAN:, cols] = parts.astype(jnp.bfloat16)


def attention(spans, seg, q, q_other, a, b):
    heads = 2 * q.shape[1] // HD
    width = heads * SPAN
    return pl.pallas_call(
        attention_kernel,
        out_shape=(
            jax.ShapeDtypeStruct((BLOCK, 2 * width), jnp.bfloat16),
            jax.ShapeDtypeStruct((TALLY, HD), jnp.float32),
        ),
        in_specs=[SMEM] + [VMEM] * 5,
        out_specs=(VMEM, VMEM),
        scratch_shapes=[
            pltpu.VMEM((16, SPAN, 2 * HD), jnp.bfloat16),
            pltpu.VMEM((2, width, HD), jnp.bfloat16),
            pltpu.SMEM((16,), jnp.int32),
            pltpu.SMEM((33,), jnp.int32),
            pltpu.VMEM((2, 1, SPAN), jnp.float32),
            pltpu.VMEM((2, 1, width), jnp.float32),
            pltpu.VMEM((2, 1, width), jnp.float32),
            pltpu.VMEM((2, HD, width), jnp.float32),
        ],
        compiler_params=grant(12),
        name="attend",
    )(spans, seg, q, q_other, a, b)


def multiply(first, heads_ref, w_ref, other_ref, out_ref):
    depth = w_ref.shape[0]
    blocks = column_blocks(lax.axis_index("tensor"))
    for g in range(out_ref.shape[0]):
        at = pl.multiple_of(blocks[first + g] * COLS, COLS)
        total = jnp.dot(heads_ref[:, :depth], w_ref[:, pl.ds(at, COLS)], preferred_element_type=jnp.float32)
        total += jnp.dot(heads_ref[:, depth:], other_ref[first + g], preferred_element_type=jnp.float32)
        out_ref[g] = total.astype(jnp.bfloat16)


def join_kernel(mine_ref, theirs_ref, w_ref, other_ref, heads_ref, out_ref):
    f32 = jnp.float32
    width = mine_ref.shape[1] // 2
    heads = width // SPAN

    def log(ref, at):
        rows = ref[SPAN:, at : at + SPAN].astype(f32)
        return rows[0:1] + rows[1:2] + rows[2:3]

    for i in range(2):
        for h in range(heads):
            a = i * width + h * SPAN
            b = i * width + (h + heads // 2) % heads * SPAN
            log_a, log_b = log(mine_ref, a), log(theirs_ref, b)
            top = jnp.maximum(log_a, log_b)
            part_a, part_b = jnp.exp2(log_a - top), jnp.exp2(log_b - top)
            total = part_a + part_b
            joined = mine_ref[:SPAN, a : a + SPAN].astype(f32) * (part_a / total)
            joined += theirs_ref[:SPAN, b : b + SPAN].astype(f32) * (part_b / total)
            heads_ref[i * SPAN : (i + 1) * SPAN, h * HD : (h + 1) * HD] = joined.T.astype(jnp.bfloat16)
    multiply(0, heads_ref, w_ref, other_ref, out_ref)


def join(mine, theirs, w, other):
    rows, depth = 2 * SPAN, 2 * w.shape[0]
    return pl.pallas_call(
        join_kernel,
        out_shape=(
            jax.ShapeDtypeStruct((rows, depth), jnp.bfloat16),
            jax.ShapeDtypeStruct((2, rows, COLS), jnp.bfloat16),
        ),
        in_specs=[VMEM] * 4,
        out_specs=(VMEM, VMEM),
        compiler_params=grant(20),
        name="join",
    )(mine, theirs, w, other)


def project_kernel(heads_ref, w_ref, other_ref, out_ref):
    multiply(2, heads_ref, w_ref, other_ref, out_ref)


def project(heads, w, other):
    rows = heads.shape[0]
    return pl.pallas_call(
        project_kernel,
        out_shape=jax.ShapeDtypeStruct((6, rows, COLS), jnp.bfloat16),
        in_specs=[VMEM] * 3,
        out_specs=VMEM,
        compiler_params=grant(20),
        name="project",
    )(heads, w, other)


def add(a, b):
    return (a.astype(jnp.float32) + b.astype(jnp.float32)).astype(jnp.bfloat16)


def per_device(queries, keys, values, out_weight, segment_ids, loss_mask, span_order):
    both = ("context", "tensor")
    f32 = jnp.float32
    cat = lambda *a: jnp.concatenate(a, axis=0)
    along_x = [[x * NZ + z for x in range(NX)] for z in range(NZ)]
    gather = lambda a: lax.all_gather(a, "context", axis=0, tiled=True, axis_index_groups=along_x)

    in_hbm = lambda a: pltpu.with_memory_space_constraint(a, pltpu.HBM)

    kv1 = prepare(in_hbm(keys), in_hbm(values), in_hbm(loss_mask))
    r1 = lax.ppermute(kv1, both, perm_context("z", inner))
    near = gather(kv1)
    r2 = lax.ppermute(cat(kv1, r1), both, perm_context("z", outer))
    q_other = lax.ppermute(queries[0], "tensor", SWAP)
    packed = pack(in_hbm(out_weight))
    weight_other = lax.ppermute(packed, "tensor", SWAP)
    far = gather(cat(r1, r2))
    mine, tally = attention(span_order, segment_ids.reshape(32, SPAN), queries[0], q_other, near, far)
    theirs = lax.ppermute(mine, "tensor", SWAP)

    inward, outward = perm_tensor(inner), perm_tensor(outer)
    heads, far = join(mine, theirs, out_weight, weight_other)
    far = lax.ppermute(far, "tensor", outward)
    rest = project(heads, out_weight, weight_other)
    around = [(d * 16 + t, (d + 1 + t % 2) % 3 * 16 + t) for d in range(3) for t in range(16)]
    one = lax.ppermute(tally, ("dp", "tensor"), around)
    two = lax.ppermute(one, "tensor", SWAP)
    mid = lax.ppermute(add(rest[0:2], far), "tensor", inward)
    near = lax.ppermute(add(rest[2:4], mid), "tensor", outward)
    last = lax.ppermute(add(rest[4], near[0]), "tensor", inward)
    count = (tally + one + two)[0, 0]
    scale_all = lax.axis_size("dp") * lax.axis_size("context") * queries.shape[1]
    weight = loss_mask[0].astype(f32) * scale_all / count
    summed = rest[5].astype(f32) + near[1].astype(f32) + last.astype(f32)
    return (summed * weight[:, None]).astype(jnp.bfloat16)[None]


def solution(mesh):
    in_specs = (
        P("dp", "context", "tensor"),
        P("dp", "context", None),
        P("dp", "context", None),
        P("tensor", None),
        P("dp", None),
        P("dp", "context"),
        P(),
    )
    out_specs = P("dp", "context", "tensor")
    return jax.shard_map(
        per_device, mesh=mesh, in_specs=in_specs, out_specs=out_specs, check_vma=False
    )
```

```python
import jax
import jax.numpy as jnp
from jax import lax
from jax.experimental import pallas as pl
from jax.experimental.pallas import tpu as pltpu
from jax.sharding import PartitionSpec as P


HD = 128
SPAN = 128
TALLY = 8
BLOCK = SPAN + TALLY
COLS = 512
LOG2E = 1.4426950408889634
LOW = -1e30


NX, NZ, NY, NC = 4, 4, 8, 2


def inner(i, c, n):
    return ((((i - c) & (n - 1)) ^ 1) + c) & (n - 1)


def outer(i, c, n):
    v = (i - c) & (n - 1)
    return (v + 2 * (v & 1) - 1 + c) & (n - 1)


def perm_context(axis, partner):
    out = []
    for x in range(NX):
        for z in range(NZ):
            for y in range(NY):
                for c in range(NC):
                    px = partner(x, c, NX) if axis == "x" else x
                    pz = partner(z, c, NZ) if axis == "z" else z
                    tensor = y * NC + c
                    out.append(((x * NZ + z) * 16 + tensor, (px * NZ + pz) * 16 + tensor))
    return out


def perm_tensor(partner):
    return [
        (y * NC + c, partner(y, c, NY) * NC + c) for y in range(NY) for c in range(NC)
    ]


SWAP = [(t, t ^ 1) for t in range(16)]


def gathered_slot(context, core, i):
    def known(at, n):
        far = outer(at, core, n)
        return (at, inner(at, core, n), far, inner(far, core, n))

    x = known(context >> 2, NX)[i // NZ]
    z = known(context & (NZ - 1), NZ)[i % NZ]
    return 2 * (x * NZ + z) + core


def column_blocks(tensor):
    y, core = tensor >> 1, tensor & 1
    v = (y - core) & (NY - 1)
    k, s = v >> 1, v & 1
    far, mid, near = (k + 2) & 3, (k + 1 - 2 * s) & 3, (k - 1 + 2 * s) & 3
    order = (2 * far + s, 2 * far + 1 - s, 2 * mid + 1 - s, 2 * mid + s)
    order += (2 * near + s, 2 * near + 1 - s, 2 * k + 1 - s, 2 * k + s)
    return [2 * ((b + core) & (NY - 1)) + core for b in order]


SMEM = pl.BlockSpec(memory_space=pltpu.SMEM)
VMEM = pl.BlockSpec(memory_space=pltpu.VMEM)
HBM = pl.BlockSpec(memory_space=pltpu.HBM)


def grant(mib):
    return pltpu.CompilerParams(vmem_limit_bytes=mib * 2**20)


def prepare_kernel(k_ref, v_ref, mask_hbm, out_ref, mask_ref, sems):
    counted = pltpu.make_async_copy(mask_hbm, mask_ref, sems.at[2])
    counted.start()
    tensor = lax.axis_index("tensor")
    rows = pl.ds(pl.multiple_of(lax.rem(tensor, NC) * SPAN, SPAN), SPAN)
    cols = pl.ds(pl.multiple_of(lax.div(tensor, NC) * HD, HD), HD)
    copies = []
    for i, ref in enumerate((k_ref, v_ref)):
        into = out_ref.at[pl.ds(0, SPAN), pl.ds(i * HD, HD)]
        copies.append(pltpu.make_async_copy(ref.at[0, rows, cols], into, sems.at[i]))
        copies[-1].start()
    counted.wait()
    total = jnp.sum(mask_ref[...].astype(jnp.float32), axis=1, keepdims=True)
    out_ref[SPAN:, :] = jnp.broadcast_to(total, (TALLY, 2 * HD)).astype(jnp.bfloat16)
    for copy in copies:
        copy.wait()


def prepare(keys, values, loss_mask):
    return pl.pallas_call(
        prepare_kernel,
        out_shape=jax.ShapeDtypeStruct((BLOCK, 2 * HD), jnp.bfloat16),
        in_specs=[HBM] * 3,
        out_specs=VMEM,
        scratch_shapes=[pltpu.VMEM(loss_mask.shape, loss_mask.dtype), pltpu.SemaphoreType.DMA((3,))],
        compiler_params=grant(2),
        name="prepare",
    )(keys, values, loss_mask)


def pack_kernel(w_ref, out_ref, sems):
    copies = []
    for g, block in enumerate(column_blocks(lax.axis_index("tensor") ^ 1)):
        at = pl.multiple_of(block * COLS, COLS)
        copies.append(pltpu.make_async_copy(w_ref.at[:, pl.ds(at, COLS)], out_ref.at[g], sems.at[g]))
        copies[-1].start()
    for copy in copies:
        copy.wait()


def pack(w):
    return pl.pallas_call(
        pack_kernel,
        out_shape=jax.ShapeDtypeStruct((8, w.shape[0], COLS), w.dtype),
        in_specs=[HBM],
        out_specs=HBM,
        scratch_shapes=[pltpu.SemaphoreType.DMA((8,))],
        compiler_params=grant(2),
        name="pack",
    )(w)


def attend(first_block, spans, blocks_ref, q8, lo_ref, m_ref, l_ref, acc, kv, places, items):
    f32 = jnp.float32
    context = lax.axis_index("context")
    core = lax.rem(lax.axis_index("tensor"), NC)
    width = q8.shape[1]
    count = jnp.int32(0)
    for b in range(8):
        kv[b] = blocks_ref[b * BLOCK : b * BLOCK + SPAN, :]
        places[b] = spans[gathered_slot(context, core, first_block + b)]
    for i in range(2):
        first = jnp.min(lo_ref[i]).astype(jnp.int32)
        q_pos = spans[2 * context + i]
        for b in range(8):
            items[count] = i * 8 + b
            seen = (places[b] <= q_pos) & ((places[b] + 1) * SPAN > first)
            count = count + seen.astype(jnp.int32)

    def step(j, carry):
        item = items[j]
        i, b = lax.shift_right_logical(item, 3), item & 7
        pos = lax.broadcasted_iota(jnp.int32, (SPAN, SPAN), 0) + places[b] * SPAN
        hi = lax.broadcasted_iota(jnp.int32, (SPAN, SPAN), 1) + spans[2 * context + i] * SPAN
        bias = jnp.where((pos.astype(f32) >= lo_ref[i]) & (pos <= hi), 0.0, LOW)
        s = lax.dot_general(kv[b, :, :HD], q8[i], (((1,), (1,)), ((), ())), preferred_element_type=f32)
        s = s * (HD ** (-0.5) * LOG2E) + jnp.concatenate([bias] * (width // SPAN), axis=1)
        old = m_ref[i]
        new = jnp.maximum(old, jnp.max(s, axis=0, keepdims=True))
        alpha = jnp.exp2(old - new)
        p = jnp.exp2(s - new)
        m_ref[i] = new
        l_ref[i] = l_ref[i] * alpha + jnp.sum(p, axis=0, keepdims=True)
        add = lax.dot_general(
            kv[b, :, HD:], p.astype(jnp.bfloat16), (((0,), (0,)), ((), ())), preferred_element_type=f32
        )
        acc[i] = acc[i] * alpha + add
        return carry

    lax.fori_loop(0, count, step, 0)
    tally = jnp.zeros((TALLY, HD), f32)
    for b in range(8):
        tally += blocks_ref[b * BLOCK + SPAN : (b + 1) * BLOCK, :HD].astype(f32)
    return tally


def first_kernel(
    spans, seg_ref, q_ref, q_other_ref, blocks_ref, q8, lo_ref, m_ref, l_ref, acc, tally_ref, kv, places, items
):
    f32 = jnp.float32
    context = lax.axis_index("context")
    heads = q8.shape[1] // SPAN
    half = heads // 2
    seg = seg_ref[...]
    starts = [jnp.sum((seg < d).astype(f32), keepdims=True) for d in range(1, 8)]
    for i in range(2):
        for h in range(heads):
            ref = q_ref if h < half else q_other_ref
            q8[i, h * SPAN : (h + 1) * SPAN, :] = ref[i * SPAN : (i + 1) * SPAN, h % half * HD : (h % half + 1) * HD]
        q_seg = seg_ref[pl.ds(2 * context + i, 1), :]
        lo = jnp.zeros((1, SPAN), f32)
        for d in range(1, 8):
            lo = jnp.where(q_seg == d, starts[d - 1], lo)
        lo_ref[i] = lo
    m_ref[...] = jnp.full(m_ref.shape, LOW, f32)
    l_ref[...] = jnp.zeros(l_ref.shape, f32)
    acc[...] = jnp.zeros(acc.shape, f32)
    tally_ref[...] = attend(0, spans, blocks_ref, q8, lo_ref, m_ref, l_ref, acc, kv, places, items)


def second_kernel(
    spans, blocks_ref, q8, lo_ref, m_in, l_in, acc_in, tally_in, out_ref, tally_ref, m_ref, l_ref, acc, kv, places, items
):
    f32 = jnp.float32
    width = q8.shape[1]
    m_ref[...] = m_in[...]
    l_ref[...] = l_in[...]
    acc[...] = acc_in[...]
    tally = attend(8, spans, blocks_ref, q8, lo_ref, m_ref, l_ref, acc, kv, places, items)
    tally_ref[...] = tally_in[...] + tally
    row = lax.broadcasted_iota(jnp.int32, (TALLY, width), 0)
    for i in range(2):
        cols = slice(i * width, (i + 1) * width)
        total = l_ref[i]
        total = jnp.where(total > 0, total, 1.0)
        out_ref[:SPAN, cols] = (acc[i] / total).astype(jnp.bfloat16)
        log = m_ref[i] + jnp.log(total) * LOG2E
        high = log.astype(jnp.bfloat16).astype(f32)
        mid = (log - high).astype(jnp.bfloat16).astype(f32)
        tail = log - high - mid
        parts = jnp.where(row == 0, high, jnp.where(row == 1, mid, jnp.where(row == 2, tail, 0.0)))
        out_ref[SPAN:, cols] = parts.astype(jnp.bfloat16)


def attention(spans, seg, q, q_other, blocks, more_blocks):
    heads = 2 * q.shape[1] // HD
    width = heads * SPAN
    f32 = jnp.float32
    state = [((2, 1, width), f32), ((2, 1, width), f32), ((2, HD, width), f32)]
    made = [((2, width, HD), jnp.bfloat16), ((2, 1, SPAN), f32), *state, ((TALLY, HD), f32)]
    scratch = [
        pltpu.VMEM((8, SPAN, 2 * HD), jnp.bfloat16),
        pltpu.SMEM((8,), jnp.int32),
        pltpu.SMEM((17,), jnp.int32),
    ]
    made = pl.pallas_call(
        first_kernel,
        out_shape=tuple(jax.ShapeDtypeStruct(*m) for m in made),
        in_specs=[SMEM] + [VMEM] * 4,
        out_specs=(VMEM,) * 6,
        scratch_shapes=scratch,
        compiler_params=grant(12),
        name="attend_first",
    )(spans, seg, q, q_other, blocks)
    return pl.pallas_call(
        second_kernel,
        out_shape=(
            jax.ShapeDtypeStruct((BLOCK, 2 * width), jnp.bfloat16),
            jax.ShapeDtypeStruct((TALLY, HD), f32),
        ),
        in_specs=[SMEM] + [VMEM] * 7,
        out_specs=(VMEM, VMEM),
        scratch_shapes=[pltpu.VMEM(*m) for m in state] + scratch,
        compiler_params=grant(12),
        name="attend_second",
    )(spans, more_blocks, *made)


def multiply(first, heads_ref, w_ref, other_ref, out_ref):
    depth = w_ref.shape[0]
    blocks = column_blocks(lax.axis_index("tensor"))
    for g in range(out_ref.shape[0]):
        at = pl.multiple_of(blocks[first + g] * COLS, COLS)
        total = jnp.dot(heads_ref[:, :depth], w_ref[:, pl.ds(at, COLS)], preferred_element_type=jnp.float32)
        total += jnp.dot(heads_ref[:, depth:], other_ref[first + g], preferred_element_type=jnp.float32)
        out_ref[g] = total.astype(jnp.bfloat16)


def join_kernel(mine_ref, theirs_ref, w_ref, other_ref, heads_ref, out_ref):
    f32 = jnp.float32
    width = mine_ref.shape[1] // 2
    heads = width // SPAN

    def log(ref, at):
        rows = ref[SPAN:, at : at + SPAN].astype(f32)
        return rows[0:1] + rows[1:2] + rows[2:3]

    for i in range(2):
        for h in range(heads):
            a = i * width + h * SPAN
            b = i * width + (h + heads // 2) % heads * SPAN
            log_a, log_b = log(mine_ref, a), log(theirs_ref, b)
            top = jnp.maximum(log_a, log_b)
            part_a, part_b = jnp.exp2(log_a - top), jnp.exp2(log_b - top)
            total = part_a + part_b
            joined = mine_ref[:SPAN, a : a + SPAN].astype(f32) * (part_a / total)
            joined += theirs_ref[:SPAN, b : b + SPAN].astype(f32) * (part_b / total)
            heads_ref[i * SPAN : (i + 1) * SPAN, h * HD : (h + 1) * HD] = joined.T.astype(jnp.bfloat16)
    multiply(0, heads_ref, w_ref, other_ref, out_ref)


def join(mine, theirs, w, other):
    rows, depth = 2 * SPAN, 2 * w.shape[0]
    return pl.pallas_call(
        join_kernel,
        out_shape=(
            jax.ShapeDtypeStruct((rows, depth), jnp.bfloat16),
            jax.ShapeDtypeStruct((2, rows, COLS), jnp.bfloat16),
        ),
        in_specs=[VMEM] * 4,
        out_specs=(VMEM, VMEM),
        compiler_params=grant(20),
        name="join",
    )(mine, theirs, w, other)


def project_kernel(heads_ref, w_ref, other_ref, out_ref):
    multiply(2, heads_ref, w_ref, other_ref, out_ref)


def project(heads, w, other):
    rows = heads.shape[0]
    return pl.pallas_call(
        project_kernel,
        out_shape=jax.ShapeDtypeStruct((6, rows, COLS), jnp.bfloat16),
        in_specs=[VMEM] * 3,
        out_specs=VMEM,
        compiler_params=grant(20),
        name="project",
    )(heads, w, other)


def add(a, b):
    return (a.astype(jnp.float32) + b.astype(jnp.float32)).astype(jnp.bfloat16)


def per_device(queries, keys, values, out_weight, segment_ids, loss_mask, span_order):
    both = ("context", "tensor")
    f32 = jnp.float32
    cat = lambda *a: jnp.concatenate(a, axis=0)
    in_hbm = lambda a: pltpu.with_memory_space_constraint(a, pltpu.HBM)

    kv1 = prepare(in_hbm(keys), in_hbm(values), in_hbm(loss_mask))
    r1 = lax.ppermute(kv1, both, perm_context("z", inner))
    q_other = lax.ppermute(queries[0], "tensor", SWAP)
    packed = pack(in_hbm(out_weight))
    kv2 = cat(kv1, r1)
    kv4 = cat(kv2, lax.ppermute(kv2, both, perm_context("z", outer)))
    weight_other = lax.ppermute(packed, "tensor", SWAP)
    kv8 = cat(kv4, lax.ppermute(kv4, both, perm_context("x", inner)))
    r8 = lax.ppermute(kv8, both, perm_context("x", outer))
    mine, tally = attention(span_order, segment_ids.reshape(32, SPAN), queries[0], q_other, kv8, r8)
    theirs = lax.ppermute(mine, "tensor", SWAP)

    inward, outward = perm_tensor(inner), perm_tensor(outer)
    heads, far = join(mine, theirs, out_weight, weight_other)
    far = lax.ppermute(far, "tensor", outward)
    rest = project(heads, out_weight, weight_other)
    around = [(d * 16 + t, (d + 1 + t % 2) % 3 * 16 + t) for d in range(3) for t in range(16)]
    one = lax.ppermute(tally, ("dp", "tensor"), around)
    two = lax.ppermute(one, "tensor", SWAP)
    mid = lax.ppermute(add(rest[0:2], far), "tensor", inward)
    near = lax.ppermute(add(rest[2:4], mid), "tensor", outward)
    last = lax.ppermute(add(rest[4], near[0]), "tensor", inward)
    count = (tally + one + two)[0, 0]
    scale_all = lax.axis_size("dp") * lax.axis_size("context") * queries.shape[1]
    weight = loss_mask[0].astype(f32) * scale_all / count
    summed = rest[5].astype(f32) + near[1].astype(f32) + last.astype(f32)
    return (summed * weight[:, None]).astype(jnp.bfloat16)[None]


def solution(mesh):
    in_specs = (
        P("dp", "context", "tensor"),
        P("dp", "context", None),
        P("dp", "context", None),
        P("tensor", None),
        P("dp", None),
        P("dp", "context"),
        P(),
    )
    out_specs = P("dp", "context", "tensor")
    return jax.shard_map(
        per_device, mesh=mesh, in_specs=in_specs, out_specs=out_specs, check_vma=False
    )
```

```python
import jax
import jax.numpy as jnp
from jax import lax
from jax.experimental import pallas as pl
from jax.experimental.pallas import tpu as pltpu
from jax.sharding import PartitionSpec as P


HD = 128
SPAN = 128
TALLY = 8
BLOCK = SPAN + TALLY
COLS = 512
LOG2E = 1.4426950408889634
LOW = -1e30


NX, NZ, NY, NC = 4, 4, 8, 2


def inner(i, c, n):
    return ((((i - c) & (n - 1)) ^ 1) + c) & (n - 1)


def outer(i, c, n):
    v = (i - c) & (n - 1)
    return (v + 2 * (v & 1) - 1 + c) & (n - 1)


def perm_context(axis, partner):
    out = []
    for x in range(NX):
        for z in range(NZ):
            for y in range(NY):
                for c in range(NC):
                    px = partner(x, c, NX) if axis == "x" else x
                    pz = partner(z, c, NZ) if axis == "z" else z
                    tensor = y * NC + c
                    out.append(((x * NZ + z) * 16 + tensor, (px * NZ + pz) * 16 + tensor))
    return out


def perm_tensor(partner):
    return [
        (y * NC + c, partner(y, c, NY) * NC + c) for y in range(NY) for c in range(NC)
    ]


SWAP = [(t, t ^ 1) for t in range(16)]


def gathered_slot(context, core, i):
    def known(at, n):
        far = outer(at, core, n)
        return (at, inner(at, core, n), far, inner(far, core, n))

    x = known(context >> 2, NX)[i // NZ]
    z = known(context & (NZ - 1), NZ)[i % NZ]
    return 2 * (x * NZ + z) + core


def column_blocks(tensor):
    y, core = tensor >> 1, tensor & 1
    v = (y - core) & (NY - 1)
    k, s = v >> 1, v & 1
    far, mid, near = (k + 2) & 3, (k + 1 - 2 * s) & 3, (k - 1 + 2 * s) & 3
    order = (2 * far + s, 2 * far + 1 - s, 2 * mid + 1 - s, 2 * mid + s)
    order += (2 * near + s, 2 * near + 1 - s, 2 * k + 1 - s, 2 * k + s)
    return [2 * ((b + core) & (NY - 1)) + core for b in order]


SMEM = pl.BlockSpec(memory_space=pltpu.SMEM)
VMEM = pl.BlockSpec(memory_space=pltpu.VMEM)
HBM = pl.BlockSpec(memory_space=pltpu.HBM)


def grant(mib):
    return pltpu.CompilerParams(vmem_limit_bytes=mib * 2**20)


def prepare_kernel(k_ref, v_ref, mask_hbm, out_ref, mask_ref, sems):
    counted = pltpu.make_async_copy(mask_hbm, mask_ref, sems.at[2])
    counted.start()
    tensor = lax.axis_index("tensor")
    rows = pl.ds(pl.multiple_of(lax.rem(tensor, NC) * SPAN, SPAN), SPAN)
    cols = pl.ds(pl.multiple_of(lax.div(tensor, NC) * HD, HD), HD)
    copies = []
    for i, ref in enumerate((k_ref, v_ref)):
        into = out_ref.at[pl.ds(0, SPAN), pl.ds(i * HD, HD)]
        copies.append(pltpu.make_async_copy(ref.at[0, rows, cols], into, sems.at[i]))
        copies[-1].start()
    counted.wait()
    total = jnp.sum(mask_ref[...].astype(jnp.float32), axis=1, keepdims=True)
    out_ref[SPAN:, :] = jnp.broadcast_to(total, (TALLY, 2 * HD)).astype(jnp.bfloat16)
    for copy in copies:
        copy.wait()


def prepare(keys, values, loss_mask):
    return pl.pallas_call(
        prepare_kernel,
        out_shape=jax.ShapeDtypeStruct((BLOCK, 2 * HD), jnp.bfloat16),
        in_specs=[HBM] * 3,
        out_specs=VMEM,
        scratch_shapes=[pltpu.VMEM(loss_mask.shape, loss_mask.dtype), pltpu.SemaphoreType.DMA((3,))],
        compiler_params=grant(2),
        name="prepare",
    )(keys, values, loss_mask)


def pack_kernel(w_ref, out_ref, sems):
    copies = []
    for g, block in enumerate(column_blocks(lax.axis_index("tensor") ^ 1)):
        at = pl.multiple_of(block * COLS, COLS)
        copies.append(pltpu.make_async_copy(w_ref.at[:, pl.ds(at, COLS)], out_ref.at[g], sems.at[g]))
        copies[-1].start()
    for copy in copies:
        copy.wait()


def pack(w):
    return pl.pallas_call(
        pack_kernel,
        out_shape=jax.ShapeDtypeStruct((8, w.shape[0], COLS), w.dtype),
        in_specs=[HBM],
        out_specs=HBM,
        scratch_shapes=[pltpu.SemaphoreType.DMA((8,))],
        compiler_params=grant(2),
        name="pack",
    )(w)


def attend(first_block, spans, blocks_ref, q8, lo_ref, m_ref, l_ref, acc, k_pair, v_pair, places, items):
    f32 = jnp.float32
    context = lax.axis_index("context")
    core = lax.rem(lax.axis_index("tensor"), NC)
    width = q8.shape[1]
    for b in range(8):
        k_pair[b] = blocks_ref[b * BLOCK : b * BLOCK + SPAN, :HD]
        v_pair[b] = blocks_ref[b * BLOCK : b * BLOCK + SPAN, HD:]
        places[b] = spans[gathered_slot(context, core, first_block + b)]
    places[8] = 1 << 20
    k_pair[8] = jnp.zeros((SPAN, HD), jnp.bfloat16)
    v_pair[8] = jnp.zeros((SPAN, HD), jnp.bfloat16)

    for i in range(2):
        first = jnp.min(lo_ref[i]).astype(jnp.int32)
        q_pos = spans[2 * context + i]
        count = jnp.int32(0)
        for b in range(8):
            items[count] = b
            seen = (places[b] <= q_pos) & ((places[b] + 1) * SPAN > first)
            count = count + seen.astype(jnp.int32)
        items[count] = 8
        hi = lax.broadcasted_iota(jnp.int32, (SPAN, SPAN), 1) + q_pos * SPAN
        row = lax.broadcasted_iota(jnp.int32, (SPAN, SPAN), 0)

        def bias(place):
            pos = row + place * SPAN
            return jnp.where((pos.astype(f32) >= lo_ref[i]) & (pos <= hi), 0.0, LOW)

        def step(j, carry):
            b, c = items[2 * j], items[2 * j + 1]
            both = jnp.concatenate([bias(places[b]), bias(places[c])], axis=0)
            k = jnp.concatenate([k_pair[b], k_pair[c]], axis=0)
            v = jnp.concatenate([v_pair[b], v_pair[c]], axis=0)
            s = lax.dot_general(k, q8[i], (((1,), (1,)), ((), ())), preferred_element_type=f32)
            s = s * (HD ** (-0.5) * LOG2E) + jnp.concatenate([both] * (width // SPAN), axis=1)
            old = m_ref[i]
            new = jnp.maximum(old, jnp.max(s, axis=0, keepdims=True))
            alpha = jnp.exp2(old - new)
            p = jnp.exp2(s - new)
            m_ref[i] = new
            l_ref[i] = l_ref[i] * alpha + jnp.sum(p, axis=0, keepdims=True)
            add = lax.dot_general(
                v, p.astype(jnp.bfloat16), (((0,), (0,)), ((), ())), preferred_element_type=f32
            )
            acc[i] = acc[i] * alpha + add
            return carry

        lax.fori_loop(0, lax.shift_right_logical(count + 1, 1), step, 0)
    tally = jnp.zeros((TALLY, HD), f32)
    for b in range(8):
        tally += blocks_ref[b * BLOCK + SPAN : (b + 1) * BLOCK, :HD].astype(f32)
    return tally


def first_kernel(
    spans, seg_ref, q_ref, q_other_ref, blocks_ref, q8, lo_ref, m_ref, l_ref, acc, tally_ref, k_pair, v_pair, places, items
):
    f32 = jnp.float32
    context = lax.axis_index("context")
    heads = q8.shape[1] // SPAN
    half = heads // 2
    seg = seg_ref[...]
    starts = [jnp.sum((seg < d).astype(f32), keepdims=True) for d in range(1, 8)]
    for i in range(2):
        for h in range(heads):
            ref = q_ref if h < half else q_other_ref
            q8[i, h * SPAN : (h + 1) * SPAN, :] = ref[i * SPAN : (i + 1) * SPAN, h % half * HD : (h % half + 1) * HD]
        q_seg = seg_ref[pl.ds(2 * context + i, 1), :]
        lo = jnp.zeros((1, SPAN), f32)
        for d in range(1, 8):
            lo = jnp.where(q_seg == d, starts[d - 1], lo)
        lo_ref[i] = lo
    m_ref[...] = jnp.full(m_ref.shape, LOW, f32)
    l_ref[...] = jnp.zeros(l_ref.shape, f32)
    acc[...] = jnp.zeros(acc.shape, f32)
    tally_ref[...] = attend(0, spans, blocks_ref, q8, lo_ref, m_ref, l_ref, acc, k_pair, v_pair, places, items)


def second_kernel(
    spans, blocks_ref, q8, lo_ref, m_in, l_in, acc_in, tally_in, out_ref, tally_ref, m_ref, l_ref, acc, k_pair, v_pair, places, items
):
    f32 = jnp.float32
    width = q8.shape[1]
    m_ref[...] = m_in[...]
    l_ref[...] = l_in[...]
    acc[...] = acc_in[...]
    tally = attend(8, spans, blocks_ref, q8, lo_ref, m_ref, l_ref, acc, k_pair, v_pair, places, items)
    tally_ref[...] = tally_in[...] + tally
    row = lax.broadcasted_iota(jnp.int32, (TALLY, width), 0)
    for i in range(2):
        cols = slice(i * width, (i + 1) * width)
        total = l_ref[i]
        total = jnp.where(total > 0, total, 1.0)
        out_ref[:SPAN, cols] = (acc[i] / total).astype(jnp.bfloat16)
        log = m_ref[i] + jnp.log(total) * LOG2E
        high = log.astype(jnp.bfloat16).astype(f32)
        mid = (log - high).astype(jnp.bfloat16).astype(f32)
        tail = log - high - mid
        parts = jnp.where(row == 0, high, jnp.where(row == 1, mid, jnp.where(row == 2, tail, 0.0)))
        out_ref[SPAN:, cols] = parts.astype(jnp.bfloat16)


def attention(spans, seg, q, q_other, blocks, more_blocks):
    heads = 2 * q.shape[1] // HD
    width = heads * SPAN
    f32 = jnp.float32
    state = [((2, 1, width), f32), ((2, 1, width), f32), ((2, HD, width), f32)]
    made = [((2, width, HD), jnp.bfloat16), ((2, 1, SPAN), f32), *state, ((TALLY, HD), f32)]
    scratch = [
        pltpu.VMEM((9, SPAN, HD), jnp.bfloat16),
        pltpu.VMEM((9, SPAN, HD), jnp.bfloat16),
        pltpu.SMEM((9,), jnp.int32),
        pltpu.SMEM((10,), jnp.int32),
    ]
    made = pl.pallas_call(
        first_kernel,
        out_shape=tuple(jax.ShapeDtypeStruct(*m) for m in made),
        in_specs=[SMEM] + [VMEM] * 4,
        out_specs=(VMEM,) * 6,
        scratch_shapes=scratch,
        compiler_params=grant(12),
        name="attend_first",
    )(spans, seg, q, q_other, blocks)
    return pl.pallas_call(
        second_kernel,
        out_shape=(
            jax.ShapeDtypeStruct((BLOCK, 2 * width), jnp.bfloat16),
            jax.ShapeDtypeStruct((TALLY, HD), f32),
        ),
        in_specs=[SMEM] + [VMEM] * 7,
        out_specs=(VMEM, VMEM),
        scratch_shapes=[pltpu.VMEM(*m) for m in state] + scratch,
        compiler_params=grant(12),
        name="attend_second",
    )(spans, more_blocks, *made)


def multiply(first, heads_ref, w_ref, other_ref, out_ref):
    depth = w_ref.shape[0]
    blocks = column_blocks(lax.axis_index("tensor"))
    for g in range(out_ref.shape[0]):
        at = pl.multiple_of(blocks[first + g] * COLS, COLS)
        total = jnp.dot(heads_ref[:, :depth], w_ref[:, pl.ds(at, COLS)], preferred_element_type=jnp.float32)
        total += jnp.dot(heads_ref[:, depth:], other_ref[first + g], preferred_element_type=jnp.float32)
        out_ref[g] = total.astype(jnp.bfloat16)


def join_kernel(mine_ref, theirs_ref, w_ref, other_ref, heads_ref, out_ref):
    f32 = jnp.float32
    width = mine_ref.shape[1] // 2
    heads = width // SPAN

    def log(ref, at):
        rows = ref[SPAN:, at : at + SPAN].astype(f32)
        return rows[0:1] + rows[1:2] + rows[2:3]

    for i in range(2):
        for h in range(heads):
            a = i * width + h * SPAN
            b = i * width + (h + heads // 2) % heads * SPAN
            log_a, log_b = log(mine_ref, a), log(theirs_ref, b)
            top = jnp.maximum(log_a, log_b)
            part_a, part_b = jnp.exp2(log_a - top), jnp.exp2(log_b - top)
            total = part_a + part_b
            joined = mine_ref[:SPAN, a : a + SPAN].astype(f32) * (part_a / total)
            joined += theirs_ref[:SPAN, b : b + SPAN].astype(f32) * (part_b / total)
            heads_ref[i * SPAN : (i + 1) * SPAN, h * HD : (h + 1) * HD] = joined.T.astype(jnp.bfloat16)
    multiply(0, heads_ref, w_ref, other_ref, out_ref)


def join(mine, theirs, w, other):
    rows, depth = 2 * SPAN, 2 * w.shape[0]
    return pl.pallas_call(
        join_kernel,
        out_shape=(
            jax.ShapeDtypeStruct((rows, depth), jnp.bfloat16),
            jax.ShapeDtypeStruct((2, rows, COLS), jnp.bfloat16),
        ),
        in_specs=[VMEM] * 4,
        out_specs=(VMEM, VMEM),
        compiler_params=grant(20),
        name="join",
    )(mine, theirs, w, other)


def project_kernel(heads_ref, w_ref, other_ref, out_ref):
    multiply(2, heads_ref, w_ref, other_ref, out_ref)


def project(heads, w, other):
    rows = heads.shape[0]
    return pl.pallas_call(
        project_kernel,
        out_shape=jax.ShapeDtypeStruct((6, rows, COLS), jnp.bfloat16),
        in_specs=[VMEM] * 3,
        out_specs=VMEM,
        compiler_params=grant(20),
        name="project",
    )(heads, w, other)


def add(a, b):
    return (a.astype(jnp.float32) + b.astype(jnp.float32)).astype(jnp.bfloat16)


def per_device(queries, keys, values, out_weight, segment_ids, loss_mask, span_order):
    both = ("context", "tensor")
    f32 = jnp.float32
    cat = lambda *a: jnp.concatenate(a, axis=0)
    in_hbm = lambda a: pltpu.with_memory_space_constraint(a, pltpu.HBM)

    kv1 = prepare(in_hbm(keys), in_hbm(values), in_hbm(loss_mask))
    r1 = lax.ppermute(kv1, both, perm_context("z", inner))
    q_other = lax.ppermute(queries[0], "tensor", SWAP)
    packed = pack(in_hbm(out_weight))
    kv2 = cat(kv1, r1)
    kv4 = cat(kv2, lax.ppermute(kv2, both, perm_context("z", outer)))
    weight_other = lax.ppermute(packed, "tensor", SWAP)
    kv8 = cat(kv4, lax.ppermute(kv4, both, perm_context("x", inner)))
    r8 = lax.ppermute(kv8, both, perm_context("x", outer))
    mine, tally = attention(span_order, segment_ids.reshape(32, SPAN), queries[0], q_other, kv8, r8)
    theirs = lax.ppermute(mine, "tensor", SWAP)

    inward, outward = perm_tensor(inner), perm_tensor(outer)
    heads, far = join(mine, theirs, out_weight, weight_other)
    far = lax.ppermute(far, "tensor", outward)
    rest = project(heads, out_weight, weight_other)
    around = [(d * 16 + t, (d + 1 + t % 2) % 3 * 16 + t) for d in range(3) for t in range(16)]
    one = lax.ppermute(tally, ("dp", "tensor"), around)
    two = lax.ppermute(one, "tensor", SWAP)
    mid = lax.ppermute(add(rest[0:2], far), "tensor", inward)
    near = lax.ppermute(add(rest[2:4], mid), "tensor", outward)
    last = lax.ppermute(add(rest[4], near[0]), "tensor", inward)
    count = (tally + one + two)[0, 0]
    scale_all = lax.axis_size("dp") * lax.axis_size("context") * queries.shape[1]
    weight = loss_mask[0].astype(f32) * scale_all / count
    summed = rest[5].astype(f32) + near[1].astype(f32) + last.astype(f32)
    return (summed * weight[:, None]).astype(jnp.bfloat16)[None]


def solution(mesh):
    in_specs = (
        P("dp", "context", "tensor"),
        P("dp", "context", None),
        P("dp", "context", None),
        P("tensor", None),
        P("dp", None),
        P("dp", "context"),
        P(),
    )
    out_specs = P("dp", "context", "tensor")
    return jax.shard_map(
        per_device, mesh=mesh, in_specs=in_specs, out_specs=out_specs, check_vma=False
    )
```

```python
import jax
import jax.numpy as jnp
from jax import lax
from jax.experimental import pallas as pl
from jax.experimental.pallas import tpu as pltpu
from jax.sharding import PartitionSpec as P


HD = 128
SPAN = 128
TALLY = 8
BLOCK = SPAN + TALLY
COLS = 512
LOG2E = 1.4426950408889634
LOW = -1e30


NX, NZ, NY, NC = 4, 4, 8, 2


def inner(i, c, n):
    return ((((i - c) & (n - 1)) ^ 1) + c) & (n - 1)


def outer(i, c, n):
    v = (i - c) & (n - 1)
    return (v + 2 * (v & 1) - 1 + c) & (n - 1)


def perm_context(axis, partner):
    out = []
    for x in range(NX):
        for z in range(NZ):
            for y in range(NY):
                for c in range(NC):
                    px = partner(x, c, NX) if axis == "x" else x
                    pz = partner(z, c, NZ) if axis == "z" else z
                    tensor = y * NC + c
                    out.append(((x * NZ + z) * 16 + tensor, (px * NZ + pz) * 16 + tensor))
    return out


def perm_tensor(partner):
    return [
        (y * NC + c, partner(y, c, NY) * NC + c) for y in range(NY) for c in range(NC)
    ]


SWAP = [(t, t ^ 1) for t in range(16)]


def gathered_slot(context, core, i):
    def known(at, n):
        far = outer(at, core, n)
        return (at, inner(at, core, n), far, inner(far, core, n))

    x = known(context >> 2, NX)[i // NZ]
    z = known(context & (NZ - 1), NZ)[i % NZ]
    return 2 * (x * NZ + z) + core


def column_blocks(tensor):
    y, core = tensor >> 1, tensor & 1
    v = (y - core) & (NY - 1)
    k, s = v >> 1, v & 1
    far, mid, near = (k + 2) & 3, (k + 1 - 2 * s) & 3, (k - 1 + 2 * s) & 3
    order = (2 * far + s, 2 * far + 1 - s, 2 * mid + 1 - s, 2 * mid + s)
    order += (2 * near + s, 2 * near + 1 - s, 2 * k + 1 - s, 2 * k + s)
    return [2 * ((b + core) & (NY - 1)) + core for b in order]


SMEM = pl.BlockSpec(memory_space=pltpu.SMEM)
VMEM = pl.BlockSpec(memory_space=pltpu.VMEM)
HBM = pl.BlockSpec(memory_space=pltpu.HBM)


def grant(mib):
    return pltpu.CompilerParams(vmem_limit_bytes=mib * 2**20)


def prepare_kernel(k_ref, v_ref, mask_hbm, out_ref, mask_ref, sems):
    counted = pltpu.make_async_copy(mask_hbm, mask_ref, sems.at[2])
    counted.start()
    tensor = lax.axis_index("tensor")
    rows = pl.ds(pl.multiple_of(lax.rem(tensor, NC) * SPAN, SPAN), SPAN)
    cols = pl.ds(pl.multiple_of(lax.div(tensor, NC) * HD, HD), HD)
    copies = []
    for i, ref in enumerate((k_ref, v_ref)):
        into = out_ref.at[pl.ds(0, SPAN), pl.ds(i * HD, HD)]
        copies.append(pltpu.make_async_copy(ref.at[0, rows, cols], into, sems.at[i]))
        copies[-1].start()
    counted.wait()
    total = jnp.sum(mask_ref[...].astype(jnp.float32), axis=1, keepdims=True)
    out_ref[SPAN:, :] = jnp.broadcast_to(total, (TALLY, 2 * HD)).astype(jnp.bfloat16)
    for copy in copies:
        copy.wait()


def prepare(keys, values, loss_mask):
    return pl.pallas_call(
        prepare_kernel,
        out_shape=jax.ShapeDtypeStruct((BLOCK, 2 * HD), jnp.bfloat16),
        in_specs=[HBM] * 3,
        out_specs=VMEM,
        scratch_shapes=[pltpu.VMEM(loss_mask.shape, loss_mask.dtype), pltpu.SemaphoreType.DMA((3,))],
        compiler_params=grant(2),
        name="prepare",
    )(keys, values, loss_mask)


def pack_kernel(w_ref, out_ref, sems):
    copies = []
    for g, block in enumerate(column_blocks(lax.axis_index("tensor") ^ 1)):
        at = pl.multiple_of(block * COLS, COLS)
        copies.append(pltpu.make_async_copy(w_ref.at[:, pl.ds(at, COLS)], out_ref.at[g], sems.at[g]))
        copies[-1].start()
    for copy in copies:
        copy.wait()


def pack(w):
    return pl.pallas_call(
        pack_kernel,
        out_shape=jax.ShapeDtypeStruct((8, w.shape[0], COLS), w.dtype),
        in_specs=[HBM],
        out_specs=HBM,
        scratch_shapes=[pltpu.SemaphoreType.DMA((8,))],
        compiler_params=grant(2),
        name="pack",
    )(w)


def attend(first_block, spans, blocks_refs, q8, lo_ref, m_ref, l_ref, acc, k_pair, v_pair, places, items):
    f32 = jnp.float32
    context = lax.axis_index("context")
    core = lax.rem(lax.axis_index("tensor"), NC)
    width = q8.shape[1]
    blocks = len(blocks_refs) * NZ
    for b in range(blocks):
        ref, at = blocks_refs[b // NZ], b % NZ * BLOCK
        k_pair[b] = ref[at : at + SPAN, :HD]
        v_pair[b] = ref[at : at + SPAN, HD:]
        places[b] = spans[gathered_slot(context, core, first_block + b)]
    places[blocks] = 1 << 20
    k_pair[blocks] = jnp.zeros((SPAN, HD), jnp.bfloat16)
    v_pair[blocks] = jnp.zeros((SPAN, HD), jnp.bfloat16)

    for i in range(2):
        first = jnp.min(lo_ref[i]).astype(jnp.int32)
        q_pos = spans[2 * context + i]
        count = jnp.int32(0)
        for b in range(blocks):
            items[count] = b
            seen = (places[b] <= q_pos) & ((places[b] + 1) * SPAN > first)
            count = count + seen.astype(jnp.int32)
        items[count] = blocks
        hi = lax.broadcasted_iota(jnp.int32, (SPAN, SPAN), 1) + q_pos * SPAN
        row = lax.broadcasted_iota(jnp.int32, (SPAN, SPAN), 0)

        def bias(place):
            pos = row + place * SPAN
            return jnp.where((pos.astype(f32) >= lo_ref[i]) & (pos <= hi), 0.0, LOW)

        def step(j, carry):
            b, c = items[2 * j], items[2 * j + 1]
            both = jnp.concatenate([bias(places[b]), bias(places[c])], axis=0)
            k = jnp.concatenate([k_pair[b], k_pair[c]], axis=0)
            v = jnp.concatenate([v_pair[b], v_pair[c]], axis=0)
            s = lax.dot_general(k, q8[i], (((1,), (1,)), ((), ())), preferred_element_type=f32)
            s = s * (HD ** (-0.5) * LOG2E) + jnp.concatenate([both] * (width // SPAN), axis=1)
            old = m_ref[i]
            new = jnp.maximum(old, jnp.max(s, axis=0, keepdims=True))
            alpha = jnp.exp2(old - new)
            p = jnp.exp2(s - new)
            m_ref[i] = new
            l_ref[i] = l_ref[i] * alpha + jnp.sum(p, axis=0, keepdims=True)
            add = lax.dot_general(
                v, p.astype(jnp.bfloat16), (((0,), (0,)), ((), ())), preferred_element_type=f32
            )
            acc[i] = acc[i] * alpha + add
            return carry

        lax.fori_loop(0, lax.shift_right_logical(count + 1, 1), step, 0)
    tally = jnp.zeros((TALLY, HD), f32)
    for ref in blocks_refs:
        for b in range(NZ):
            tally += ref[b * BLOCK + SPAN : (b + 1) * BLOCK, :HD].astype(f32)
    return tally


def first_kernel(
    spans, seg_ref, q_ref, q_other_ref, blocks_ref, q8, lo_ref, m_ref, l_ref, acc, tally_ref, k_pair, v_pair, places, items
):
    f32 = jnp.float32
    context = lax.axis_index("context")
    heads = q8.shape[1] // SPAN
    half = heads // 2
    seg = seg_ref[...]
    starts = [jnp.sum((seg < d).astype(f32), keepdims=True) for d in range(1, 8)]
    for i in range(2):
        for h in range(heads):
            ref = q_ref if h < half else q_other_ref
            q8[i, h * SPAN : (h + 1) * SPAN, :] = ref[i * SPAN : (i + 1) * SPAN, h % half * HD : (h % half + 1) * HD]
        q_seg = seg_ref[pl.ds(2 * context + i, 1), :]
        lo = jnp.zeros((1, SPAN), f32)
        for d in range(1, 8):
            lo = jnp.where(q_seg == d, starts[d - 1], lo)
        lo_ref[i] = lo
    m_ref[...] = jnp.full(m_ref.shape, LOW, f32)
    l_ref[...] = jnp.zeros(l_ref.shape, f32)
    acc[...] = jnp.zeros(acc.shape, f32)
    tally_ref[...] = attend(0, spans, (blocks_ref,), q8, lo_ref, m_ref, l_ref, acc, k_pair, v_pair, places, items)


def second_kernel(
    spans, a_ref, b_ref, q8, lo_ref, m_in, l_in, acc_in, tally_in, m_ref, l_ref, acc, tally_ref, k_pair, v_pair, places, items
):
    m_ref[...] = m_in[...]
    l_ref[...] = l_in[...]
    acc[...] = acc_in[...]
    tally = attend(NZ, spans, (a_ref, b_ref), q8, lo_ref, m_ref, l_ref, acc, k_pair, v_pair, places, items)
    tally_ref[...] = tally_in[...] + tally


def third_kernel(
    spans, blocks_ref, q8, lo_ref, m_in, l_in, acc_in, tally_in, out_ref, tally_ref, m_ref, l_ref, acc, k_pair, v_pair, places, items
):
    f32 = jnp.float32
    width = q8.shape[1]
    m_ref[...] = m_in[...]
    l_ref[...] = l_in[...]
    acc[...] = acc_in[...]
    tally = attend(3 * NZ, spans, (blocks_ref,), q8, lo_ref, m_ref, l_ref, acc, k_pair, v_pair, places, items)
    tally_ref[...] = tally_in[...] + tally
    row = lax.broadcasted_iota(jnp.int32, (TALLY, width), 0)
    for i in range(2):
        cols = slice(i * width, (i + 1) * width)
        total = l_ref[i]
        total = jnp.where(total > 0, total, 1.0)
        out_ref[:SPAN, cols] = (acc[i] / total).astype(jnp.bfloat16)
        log = m_ref[i] + jnp.log(total) * LOG2E
        high = log.astype(jnp.bfloat16).astype(f32)
        mid = (log - high).astype(jnp.bfloat16).astype(f32)
        tail = log - high - mid
        parts = jnp.where(row == 0, high, jnp.where(row == 1, mid, jnp.where(row == 2, tail, 0.0)))
        out_ref[SPAN:, cols] = parts.astype(jnp.bfloat16)


def attention(spans, seg, q, q_other, own, inner_blocks, outer_blocks, far_blocks):
    heads = 2 * q.shape[1] // HD
    width = heads * SPAN
    f32 = jnp.float32
    state = [((2, 1, width), f32), ((2, 1, width), f32), ((2, HD, width), f32)]
    tally = ((TALLY, HD), f32)

    def call(kernel, blocks, made, kept, *operands):
        return pl.pallas_call(
            kernel,
            out_shape=tuple(jax.ShapeDtypeStruct(*m) for m in made),
            in_specs=[SMEM] + [VMEM] * (len(operands) - 1),
            out_specs=(VMEM,) * len(made),
            scratch_shapes=[pltpu.VMEM(*m) for m in kept]
            + [
                pltpu.VMEM((blocks + 1, SPAN, HD), jnp.bfloat16),
                pltpu.VMEM((blocks + 1, SPAN, HD), jnp.bfloat16),
                pltpu.SMEM((blocks + 1,), jnp.int32),
                pltpu.SMEM((blocks + 2,), jnp.int32),
            ],
            compiler_params=grant(12),
        )(*operands)

    made = [((2, width, HD), jnp.bfloat16), ((2, 1, SPAN), f32), *state, tally]
    q8, lo, *running = call(first_kernel, NZ, made, [], spans, seg, q, q_other, own)
    running = call(second_kernel, 2 * NZ, [*state, tally], [], spans, inner_blocks, outer_blocks, q8, lo, *running)
    made = [((BLOCK, 2 * width), jnp.bfloat16), tally]
    return call(third_kernel, NZ, made, state, spans, far_blocks, q8, lo, *running)


def multiply(first, heads_ref, w_ref, other_ref, out_ref):
    depth = w_ref.shape[0]
    blocks = column_blocks(lax.axis_index("tensor"))
    for g in range(out_ref.shape[0]):
        at = pl.multiple_of(blocks[first + g] * COLS, COLS)
        total = jnp.dot(heads_ref[:, :depth], w_ref[:, pl.ds(at, COLS)], preferred_element_type=jnp.float32)
        total += jnp.dot(heads_ref[:, depth:], other_ref[first + g], preferred_element_type=jnp.float32)
        out_ref[g] = total.astype(jnp.bfloat16)


def join_kernel(mine_ref, theirs_ref, w_ref, other_ref, heads_ref, out_ref):
    f32 = jnp.float32
    width = mine_ref.shape[1] // 2
    heads = width // SPAN

    def log(ref, at):
        rows = ref[SPAN:, at : at + SPAN].astype(f32)
        return rows[0:1] + rows[1:2] + rows[2:3]

    for i in range(2):
        for h in range(heads):
            a = i * width + h * SPAN
            b = i * width + (h + heads // 2) % heads * SPAN
            log_a, log_b = log(mine_ref, a), log(theirs_ref, b)
            top = jnp.maximum(log_a, log_b)
            part_a, part_b = jnp.exp2(log_a - top), jnp.exp2(log_b - top)
            total = part_a + part_b
            joined = mine_ref[:SPAN, a : a + SPAN].astype(f32) * (part_a / total)
            joined += theirs_ref[:SPAN, b : b + SPAN].astype(f32) * (part_b / total)
            heads_ref[i * SPAN : (i + 1) * SPAN, h * HD : (h + 1) * HD] = joined.T.astype(jnp.bfloat16)
    multiply(0, heads_ref, w_ref, other_ref, out_ref)


def join(mine, theirs, w, other):
    rows, depth = 2 * SPAN, 2 * w.shape[0]
    return pl.pallas_call(
        join_kernel,
        out_shape=(
            jax.ShapeDtypeStruct((rows, depth), jnp.bfloat16),
            jax.ShapeDtypeStruct((2, rows, COLS), jnp.bfloat16),
        ),
        in_specs=[VMEM] * 4,
        out_specs=(VMEM, VMEM),
        compiler_params=grant(20),
        name="join",
    )(mine, theirs, w, other)


def project_kernel(heads_ref, w_ref, other_ref, out_ref):
    multiply(2, heads_ref, w_ref, other_ref, out_ref)


def project(heads, w, other):
    rows = heads.shape[0]
    return pl.pallas_call(
        project_kernel,
        out_shape=jax.ShapeDtypeStruct((6, rows, COLS), jnp.bfloat16),
        in_specs=[VMEM] * 3,
        out_specs=VMEM,
        compiler_params=grant(20),
        name="project",
    )(heads, w, other)


def add(a, b):
    return (a.astype(jnp.float32) + b.astype(jnp.float32)).astype(jnp.bfloat16)


def per_device(queries, keys, values, out_weight, segment_ids, loss_mask, span_order):
    both = ("context", "tensor")
    f32 = jnp.float32
    cat = lambda *a: jnp.concatenate(a, axis=0)
    in_hbm = lambda a: pltpu.with_memory_space_constraint(a, pltpu.HBM)

    kv1 = prepare(in_hbm(keys), in_hbm(values), in_hbm(loss_mask))
    r1 = lax.ppermute(kv1, both, perm_context("z", inner))
    q_other = lax.ppermute(queries[0], "tensor", SWAP)
    packed = pack(in_hbm(out_weight))
    kv2 = cat(kv1, r1)
    kv4 = cat(kv2, lax.ppermute(kv2, both, perm_context("z", outer)))
    weight_other = lax.ppermute(packed, "tensor", SWAP)
    beyond = lambda i, c, n: inner(outer(i, c, n), c, n)
    gathered = [
        lax.ppermute(kv4, both, perm_context("x", inner)),
        lax.ppermute(kv4, both, perm_context("x", outer)),
        lax.ppermute(kv4, both, perm_context("x", beyond)),
    ]
    mine, tally = attention(span_order, segment_ids.reshape(32, SPAN), queries[0], q_other, kv4, *gathered)
    theirs = lax.ppermute(mine, "tensor", SWAP)

    inward, outward = perm_tensor(inner), perm_tensor(outer)
    heads, far = join(mine, theirs, out_weight, weight_other)
    far = lax.ppermute(far, "tensor", outward)
    rest = project(heads, out_weight, weight_other)
    around = [(d * 16 + t, (d + 1 + t % 2) % 3 * 16 + t) for d in range(3) for t in range(16)]
    early = lax.ppermute(rest[4], "tensor", inward)
    one = lax.ppermute(tally, ("dp", "tensor"), around)
    two = lax.ppermute(one, "tensor", SWAP)
    mid = lax.ppermute(add(rest[0:2], far), "tensor", inward)
    near = add(rest[2:4], mid)
    passing = lax.ppermute(near[0], "tensor", perm_tensor(beyond))
    near = lax.ppermute(near[1], "tensor", outward)
    count = (tally + one + two)[0, 0]
    scale_all = lax.axis_size("dp") * lax.axis_size("context") * queries.shape[1]
    weight = loss_mask[0].astype(f32) * scale_all / count
    summed = rest[5].astype(f32) + early.astype(f32) + near.astype(f32) + passing.astype(f32)
    return (summed * weight[:, None]).astype(jnp.bfloat16)[None]


def solution(mesh):
    in_specs = (
        P("dp", "context", "tensor"),
        P("dp", "context", None),
        P("dp", "context", None),
        P("tensor", None),
        P("dp", None),
        P("dp", "context"),
        P(),
    )
    out_specs = P("dp", "context", "tensor")
    return jax.shard_map(
        per_device, mesh=mesh, in_specs=in_specs, out_specs=out_specs, check_vma=False
    )
```

```python
import jax
import jax.numpy as jnp
from jax import lax
from jax.experimental import pallas as pl
from jax.experimental.pallas import tpu as pltpu
from jax.sharding import PartitionSpec as P


HD = 128
SPAN = 128
TALLY = 8
BLOCK = SPAN + TALLY
COLS = 512
LOG2E = 1.4426950408889634
LOW = -1e30


NX, NZ, NY, NC = 4, 4, 8, 2


def inner(i, c, n):
    return ((((i - c) & (n - 1)) ^ 1) + c) & (n - 1)


def outer(i, c, n):
    v = (i - c) & (n - 1)
    return (v + 2 * (v & 1) - 1 + c) & (n - 1)


def perm_context(axis, partner):
    out = []
    for x in range(NX):
        for z in range(NZ):
            for y in range(NY):
                for c in range(NC):
                    px = partner(x, c, NX) if axis == "x" else x
                    pz = partner(z, c, NZ) if axis == "z" else z
                    tensor = y * NC + c
                    out.append(((x * NZ + z) * 16 + tensor, (px * NZ + pz) * 16 + tensor))
    return out


def perm_tensor(partner):
    return [
        (y * NC + c, partner(y, c, NY) * NC + c) for y in range(NY) for c in range(NC)
    ]


SWAP = [(t, t ^ 1) for t in range(16)]


def gathered_slot(context, core, i):
    def known(at, n):
        far = outer(at, core, n)
        return (at, inner(at, core, n), far, inner(far, core, n))

    x = known(context >> 2, NX)[i // NZ]
    z = known(context & (NZ - 1), NZ)[i % NZ]
    return 2 * (x * NZ + z) + core


def column_blocks(tensor):
    y, core = tensor >> 1, tensor & 1
    v = (y - core) & (NY - 1)
    k, s = v >> 1, v & 1
    far, mid, near = (k + 2) & 3, (k + 1 - 2 * s) & 3, (k - 1 + 2 * s) & 3
    order = (2 * far + s, 2 * far + 1 - s, 2 * mid + 1 - s, 2 * mid + s)
    order += (2 * near + s, 2 * near + 1 - s, 2 * k + 1 - s, 2 * k + s)
    return [2 * ((b + core) & (NY - 1)) + core for b in order]


SMEM = pl.BlockSpec(memory_space=pltpu.SMEM)
VMEM = pl.BlockSpec(memory_space=pltpu.VMEM)
HBM = pl.BlockSpec(memory_space=pltpu.HBM)


def grant(mib):
    return pltpu.CompilerParams(vmem_limit_bytes=mib * 2**20)


def prepare_kernel(k_ref, v_ref, mask_hbm, out_ref, mask_ref, sems):
    counted = pltpu.make_async_copy(mask_hbm, mask_ref, sems.at[2])
    counted.start()
    tensor = lax.axis_index("tensor")
    rows = pl.ds(pl.multiple_of(lax.rem(tensor, NC) * SPAN, SPAN), SPAN)
    cols = pl.ds(pl.multiple_of(lax.div(tensor, NC) * HD, HD), HD)
    copies = []
    for i, ref in enumerate((k_ref, v_ref)):
        into = out_ref.at[pl.ds(0, SPAN), pl.ds(i * HD, HD)]
        copies.append(pltpu.make_async_copy(ref.at[0, rows, cols], into, sems.at[i]))
        copies[-1].start()
    counted.wait()
    total = jnp.sum(mask_ref[...].astype(jnp.float32), axis=1, keepdims=True)
    out_ref[SPAN:, :] = jnp.broadcast_to(total, (TALLY, 2 * HD)).astype(jnp.bfloat16)
    for copy in copies:
        copy.wait()


def prepare(keys, values, loss_mask):
    return pl.pallas_call(
        prepare_kernel,
        out_shape=jax.ShapeDtypeStruct((BLOCK, 2 * HD), jnp.bfloat16),
        in_specs=[HBM] * 3,
        out_specs=VMEM,
        scratch_shapes=[pltpu.VMEM(loss_mask.shape, loss_mask.dtype), pltpu.SemaphoreType.DMA((3,))],
        compiler_params=grant(2),
        name="prepare",
    )(keys, values, loss_mask)


def pack_kernel(w_ref, out_ref, sems):
    copies = []
    for g, block in enumerate(column_blocks(lax.axis_index("tensor") ^ 1)):
        at = pl.multiple_of(block * COLS, COLS)
        copies.append(pltpu.make_async_copy(w_ref.at[:, pl.ds(at, COLS)], out_ref.at[g], sems.at[g]))
        copies[-1].start()
    for copy in copies:
        copy.wait()


def pack(w):
    return pl.pallas_call(
        pack_kernel,
        out_shape=jax.ShapeDtypeStruct((8, w.shape[0], COLS), w.dtype),
        in_specs=[HBM],
        out_specs=HBM,
        scratch_shapes=[pltpu.SemaphoreType.DMA((8,))],
        compiler_params=grant(2),
        name="pack",
    )(w)


def attend(first_block, spans, blocks_refs, q8, lo_ref, m_ref, l_ref, acc, k_pair, v_pair, places, items):
    f32 = jnp.float32
    context = lax.axis_index("context")
    core = lax.rem(lax.axis_index("tensor"), NC)
    width = q8.shape[1]
    blocks = len(blocks_refs) * NZ
    for b in range(blocks):
        ref, at = blocks_refs[b // NZ], b % NZ * BLOCK
        k_pair[b] = ref[at : at + SPAN, :HD]
        v_pair[b] = ref[at : at + SPAN, HD:]
        places[b] = spans[gathered_slot(context, core, first_block + b)]
    places[blocks] = 1 << 20
    k_pair[blocks] = jnp.zeros((SPAN, HD), jnp.bfloat16)
    v_pair[blocks] = jnp.zeros((SPAN, HD), jnp.bfloat16)

    for i in range(2):
        first = jnp.min(lo_ref[i]).astype(jnp.int32)
        q_pos = spans[2 * context + i]
        count = jnp.int32(0)
        for b in range(blocks):
            items[count] = b
            seen = (places[b] <= q_pos) & ((places[b] + 1) * SPAN > first)
            count = count + seen.astype(jnp.int32)
        items[count] = blocks
        hi = lax.broadcasted_iota(jnp.int32, (SPAN, SPAN), 1) + q_pos * SPAN
        row = lax.broadcasted_iota(jnp.int32, (SPAN, SPAN), 0)

        def bias(place):
            pos = row + place * SPAN
            return jnp.where((pos.astype(f32) >= lo_ref[i]) & (pos <= hi), 0.0, LOW)

        def step(j, carry):
            b, c = items[2 * j], items[2 * j + 1]
            both = jnp.concatenate([bias(places[b]), bias(places[c])], axis=0)
            k = jnp.concatenate([k_pair[b], k_pair[c]], axis=0)
            v = jnp.concatenate([v_pair[b], v_pair[c]], axis=0)
            s = lax.dot_general(k, q8[i], (((1,), (1,)), ((), ())), preferred_element_type=f32)
            s = s * (HD ** (-0.5) * LOG2E) + jnp.concatenate([both] * (width // SPAN), axis=1)
            old = m_ref[i]
            new = jnp.maximum(old, jnp.max(s, axis=0, keepdims=True))
            alpha = jnp.exp2(old - new)
            p = jnp.exp2(s - new)
            m_ref[i] = new
            l_ref[i] = l_ref[i] * alpha + jnp.sum(p, axis=0, keepdims=True)
            add = lax.dot_general(
                v, p.astype(jnp.bfloat16), (((0,), (0,)), ((), ())), preferred_element_type=f32
            )
            acc[i] = acc[i] * alpha + add
            return carry

        lax.fori_loop(0, lax.shift_right_logical(count + 1, 1), step, 0)
    tally = jnp.zeros((TALLY, HD), f32)
    for ref in blocks_refs:
        for b in range(NZ):
            tally += ref[b * BLOCK + SPAN : (b + 1) * BLOCK, :HD].astype(f32)
    return tally


def first_kernel(
    spans, seg_ref, q_ref, q_other_ref, blocks_ref, q8, lo_ref, m_ref, l_ref, acc, tally_ref, k_pair, v_pair, places, items
):
    f32 = jnp.float32
    context = lax.axis_index("context")
    heads = q8.shape[1] // SPAN
    half = heads // 2
    seg = seg_ref[...]
    starts = [jnp.sum((seg < d).astype(f32), keepdims=True) for d in range(1, 8)]
    for i in range(2):
        for h in range(heads):
            ref = q_ref if h < half else q_other_ref
            q8[i, h * SPAN : (h + 1) * SPAN, :] = ref[i * SPAN : (i + 1) * SPAN, h % half * HD : (h % half + 1) * HD]
        q_seg = seg_ref[pl.ds(2 * context + i, 1), :]
        lo = jnp.zeros((1, SPAN), f32)
        for d in range(1, 8):
            lo = jnp.where(q_seg == d, starts[d - 1], lo)
        lo_ref[i] = lo
    m_ref[...] = jnp.full(m_ref.shape, LOW, f32)
    l_ref[...] = jnp.zeros(l_ref.shape, f32)
    acc[...] = jnp.zeros(acc.shape, f32)
    tally_ref[...] = attend(0, spans, (blocks_ref,), q8, lo_ref, m_ref, l_ref, acc, k_pair, v_pair, places, items)


def second_kernel(
    spans, a_ref, b_ref, q8, lo_ref, m_in, l_in, acc_in, tally_in, m_ref, l_ref, acc, tally_ref, k_pair, v_pair, places, items
):
    m_ref[...] = m_in[...]
    l_ref[...] = l_in[...]
    acc[...] = acc_in[...]
    tally = attend(NZ, spans, (a_ref, b_ref), q8, lo_ref, m_ref, l_ref, acc, k_pair, v_pair, places, items)
    tally_ref[...] = tally_in[...] + tally


def third_kernel(
    spans, blocks_ref, q8, lo_ref, m_in, l_in, acc_in, tally_in, out_ref, tally_ref, m_ref, l_ref, acc, k_pair, v_pair, places, items
):
    f32 = jnp.float32
    width = q8.shape[1]
    m_ref[...] = m_in[...]
    l_ref[...] = l_in[...]
    acc[...] = acc_in[...]
    tally = attend(3 * NZ, spans, (blocks_ref,), q8, lo_ref, m_ref, l_ref, acc, k_pair, v_pair, places, items)
    tally_ref[...] = tally_in[...] + tally
    row = lax.broadcasted_iota(jnp.int32, (TALLY, width), 0)
    for i in range(2):
        cols = slice(i * width, (i + 1) * width)
        total = l_ref[i]
        total = jnp.where(total > 0, total, 1.0)
        out_ref[:SPAN, cols] = (acc[i] / total).astype(jnp.bfloat16)
        log = m_ref[i] + jnp.log(total) * LOG2E
        high = log.astype(jnp.bfloat16).astype(f32)
        mid = (log - high).astype(jnp.bfloat16).astype(f32)
        tail = log - high - mid
        parts = jnp.where(row == 0, high, jnp.where(row == 1, mid, jnp.where(row == 2, tail, 0.0)))
        out_ref[SPAN:, cols] = parts.astype(jnp.bfloat16)


def attention(spans, seg, q, q_other, own, inner_blocks, outer_blocks, far_blocks):
    heads = 2 * q.shape[1] // HD
    width = heads * SPAN
    f32 = jnp.float32
    state = [((2, 1, width), f32), ((2, 1, width), f32), ((2, HD, width), f32)]
    tally = ((TALLY, HD), f32)

    def call(kernel, blocks, made, kept, *operands):
        return pl.pallas_call(
            kernel,
            out_shape=tuple(jax.ShapeDtypeStruct(*m) for m in made),
            in_specs=[SMEM] + [VMEM] * (len(operands) - 1),
            out_specs=(VMEM,) * len(made),
            scratch_shapes=[pltpu.VMEM(*m) for m in kept]
            + [
                pltpu.VMEM((blocks + 1, SPAN, HD), jnp.bfloat16),
                pltpu.VMEM((blocks + 1, SPAN, HD), jnp.bfloat16),
                pltpu.SMEM((blocks + 1,), jnp.int32),
                pltpu.SMEM((blocks + 2,), jnp.int32),
            ],
            compiler_params=grant(12),
        )(*operands)

    made = [((2, width, HD), jnp.bfloat16), ((2, 1, SPAN), f32), *state, tally]
    q8, lo, *running = call(first_kernel, NZ, made, [], spans, seg, q, q_other, own)
    running = call(second_kernel, 2 * NZ, [*state, tally], [], spans, inner_blocks, outer_blocks, q8, lo, *running)
    made = [((BLOCK, 2 * width), jnp.bfloat16), tally]
    return call(third_kernel, NZ, made, state, spans, far_blocks, q8, lo, *running)


def multiply(first, heads_ref, w_ref, other_ref, out_refs):
    depth = w_ref.shape[0]
    blocks = column_blocks(lax.axis_index("tensor"))
    for g, out_ref in enumerate(out_refs):
        at = pl.multiple_of(blocks[first + g] * COLS, COLS)
        total = jnp.dot(heads_ref[:, :depth], w_ref[:, pl.ds(at, COLS)], preferred_element_type=jnp.float32)
        total += jnp.dot(heads_ref[:, depth:], other_ref[first + g], preferred_element_type=jnp.float32)
        out_ref[...] = total.astype(jnp.bfloat16)


def join_kernel(mine_ref, theirs_ref, w_ref, other_ref, heads_ref, *out_refs):
    f32 = jnp.float32
    width = mine_ref.shape[1] // 2
    heads = width // SPAN

    def log(ref, at):
        rows = ref[SPAN:, at : at + SPAN].astype(f32)
        return rows[0:1] + rows[1:2] + rows[2:3]

    for i in range(2):
        for h in range(heads):
            a = i * width + h * SPAN
            b = i * width + (h + heads // 2) % heads * SPAN
            log_a, log_b = log(mine_ref, a), log(theirs_ref, b)
            top = jnp.maximum(log_a, log_b)
            part_a, part_b = jnp.exp2(log_a - top), jnp.exp2(log_b - top)
            total = part_a + part_b
            joined = mine_ref[:SPAN, a : a + SPAN].astype(f32) * (part_a / total)
            joined += theirs_ref[:SPAN, b : b + SPAN].astype(f32) * (part_b / total)
            heads_ref[i * SPAN : (i + 1) * SPAN, h * HD : (h + 1) * HD] = joined.T.astype(jnp.bfloat16)
    multiply(0, heads_ref, w_ref, other_ref, out_refs)


def join(mine, theirs, w, other):
    rows, depth = 2 * SPAN, 2 * w.shape[0]
    return pl.pallas_call(
        join_kernel,
        out_shape=(
            jax.ShapeDtypeStruct((rows, depth), jnp.bfloat16),
            jax.ShapeDtypeStruct((rows, COLS), jnp.bfloat16),
            jax.ShapeDtypeStruct((rows, COLS), jnp.bfloat16),
        ),
        in_specs=[VMEM] * 4,
        out_specs=(VMEM,) * 3,
        compiler_params=grant(20),
        name="join",
    )(mine, theirs, w, other)


def project_kernel(heads_ref, w_ref, other_ref, *out_refs):
    multiply(2, heads_ref, w_ref, other_ref, out_refs)


def project(heads, w, other):
    rows = heads.shape[0]
    return pl.pallas_call(
        project_kernel,
        out_shape=(jax.ShapeDtypeStruct((rows, COLS), jnp.bfloat16),) * 6,
        in_specs=[VMEM] * 3,
        out_specs=(VMEM,) * 6,
        compiler_params=grant(20),
        name="project",
    )(heads, w, other)


def add_kernel(a_ref, b_ref, out_ref):
    out_ref[...] = (a_ref[...].astype(jnp.float32) + b_ref[...].astype(jnp.float32)).astype(jnp.bfloat16)


def add(a, b):
    return pl.pallas_call(
        add_kernel,
        out_shape=jax.ShapeDtypeStruct(a.shape, a.dtype),
        in_specs=[VMEM, VMEM],
        out_specs=VMEM,
        compiler_params=grant(4),
        name="add",
    )(a, b)


def per_device(queries, keys, values, out_weight, segment_ids, loss_mask, span_order):
    both = ("context", "tensor")
    f32 = jnp.float32
    cat = lambda *a: jnp.concatenate(a, axis=0)
    in_hbm = lambda a: pltpu.with_memory_space_constraint(a, pltpu.HBM)

    kv1 = prepare(in_hbm(keys), in_hbm(values), in_hbm(loss_mask))
    r1 = lax.ppermute(kv1, both, perm_context("z", inner))
    q_other = lax.ppermute(queries[0], "tensor", SWAP)
    packed = pack(in_hbm(out_weight))
    kv2 = cat(kv1, r1)
    kv4 = cat(kv2, lax.ppermute(kv2, both, perm_context("z", outer)))
    weight_other = lax.ppermute(packed, "tensor", SWAP)
    beyond = lambda i, c, n: inner(outer(i, c, n), c, n)
    gathered = [
        lax.ppermute(kv4, both, perm_context("x", inner)),
        lax.ppermute(kv4, both, perm_context("x", outer)),
        lax.ppermute(kv4, both, perm_context("x", beyond)),
    ]
    mine, tally = attention(span_order, segment_ids.reshape(32, SPAN), queries[0], q_other, kv4, *gathered)
    theirs = lax.ppermute(mine, "tensor", SWAP)

    inward, outward = perm_tensor(inner), perm_tensor(outer)
    heads, far_a, far_b = join(mine, theirs, out_weight, weight_other)
    far_a = lax.ppermute(far_a, "tensor", outward)
    far_b = lax.ppermute(far_b, "tensor", outward)
    mid_a, mid_b, near_a, near_b, early, own = project(heads, out_weight, weight_other)
    around = [(d * 16 + t, (d + 1 + t % 2) % 3 * 16 + t) for d in range(3) for t in range(16)]
    early = lax.ppermute(early, "tensor", inward)
    one = lax.ppermute(tally, ("dp", "tensor"), around)
    two = lax.ppermute(one, "tensor", SWAP)
    mid_a = lax.ppermute(add(mid_a, far_a), "tensor", inward)
    mid_b = lax.ppermute(add(mid_b, far_b), "tensor", inward)
    near_a = lax.ppermute(add(near_a, mid_a), "tensor", perm_tensor(beyond))
    near_b = lax.ppermute(add(near_b, mid_b), "tensor", outward)
    count = (tally + one + two)[0, 0]
    scale_all = lax.axis_size("dp") * lax.axis_size("context") * queries.shape[1]
    weight = loss_mask[0].astype(f32) * scale_all / count
    summed = own.astype(f32) + early.astype(f32) + near_a.astype(f32) + near_b.astype(f32)
    return (summed * weight[:, None]).astype(jnp.bfloat16)[None]


def solution(mesh):
    in_specs = (
        P("dp", "context", "tensor"),
        P("dp", "context", None),
        P("dp", "context", None),
        P("tensor", None),
        P("dp", None),
        P("dp", "context"),
        P(),
    )
    out_specs = P("dp", "context", "tensor")
    return jax.shard_map(
        per_device, mesh=mesh, in_specs=in_specs, out_specs=out_specs, check_vma=False
    )
```

```python
import jax
import jax.numpy as jnp
from jax import lax
from jax.experimental import pallas as pl
from jax.experimental.pallas import tpu as pltpu
from jax.sharding import PartitionSpec as P


HD = 128
SPAN = 128
TALLY = 8
BLOCK = SPAN + TALLY
COLS = 512
LOG2E = 1.4426950408889634
LOW = -1e30


NX, NZ, NY, NC = 4, 4, 8, 2


def inner(i, c, n):
    return ((((i - c) & (n - 1)) ^ 1) + c) & (n - 1)


def outer(i, c, n):
    v = (i - c) & (n - 1)
    return (v + 2 * (v & 1) - 1 + c) & (n - 1)


def perm_context(axis, partner):
    out = []
    for x in range(NX):
        for z in range(NZ):
            for y in range(NY):
                for c in range(NC):
                    px = partner(x, c, NX) if axis == "x" else x
                    pz = partner(z, c, NZ) if axis == "z" else z
                    tensor = y * NC + c
                    out.append(((x * NZ + z) * 16 + tensor, (px * NZ + pz) * 16 + tensor))
    return out


def perm_tensor(partner):
    return [
        (y * NC + c, partner(y, c, NY) * NC + c) for y in range(NY) for c in range(NC)
    ]


SWAP = [(t, t ^ 1) for t in range(16)]


def gathered_slot(context, core, i):
    def known(at, n):
        far = outer(at, core, n)
        return (at, inner(at, core, n), far, inner(far, core, n))

    x = known(context >> 2, NX)[i // NZ]
    z = known(context & (NZ - 1), NZ)[i % NZ]
    return 2 * (x * NZ + z) + core


def column_blocks(tensor):
    y, core = tensor >> 1, tensor & 1
    v = (y - core) & (NY - 1)
    k, s = v >> 1, v & 1
    far, mid, near = (k + 2) & 3, (k + 1 - 2 * s) & 3, (k - 1 + 2 * s) & 3
    order = (2 * far + s, 2 * far + 1 - s, 2 * mid + 1 - s, 2 * mid + s)
    order += (2 * near + s, 2 * near + 1 - s, 2 * k + 1 - s, 2 * k + s)
    return [2 * ((b + core) & (NY - 1)) + core for b in order]


SMEM = pl.BlockSpec(memory_space=pltpu.SMEM)
VMEM = pl.BlockSpec(memory_space=pltpu.VMEM)
HBM = pl.BlockSpec(memory_space=pltpu.HBM)


def grant(mib):
    return pltpu.CompilerParams(vmem_limit_bytes=mib * 2**20)


def prepare_kernel(k_ref, v_ref, mask_hbm, out_ref, mask_ref, sems):
    counted = pltpu.make_async_copy(mask_hbm, mask_ref, sems.at[2])
    counted.start()
    tensor = lax.axis_index("tensor")
    rows = pl.ds(pl.multiple_of(lax.rem(tensor, NC) * SPAN, SPAN), SPAN)
    cols = pl.ds(pl.multiple_of(lax.div(tensor, NC) * HD, HD), HD)
    copies = []
    for i, ref in enumerate((k_ref, v_ref)):
        into = out_ref.at[pl.ds(0, SPAN), pl.ds(i * HD, HD)]
        copies.append(pltpu.make_async_copy(ref.at[0, rows, cols], into, sems.at[i]))
        copies[-1].start()
    counted.wait()
    total = jnp.sum(mask_ref[...].astype(jnp.float32), axis=1, keepdims=True)
    out_ref[SPAN:, :] = jnp.broadcast_to(total, (TALLY, 2 * HD)).astype(jnp.bfloat16)
    for copy in copies:
        copy.wait()


def prepare(keys, values, loss_mask):
    return pl.pallas_call(
        prepare_kernel,
        out_shape=jax.ShapeDtypeStruct((BLOCK, 2 * HD), jnp.bfloat16),
        in_specs=[HBM] * 3,
        out_specs=VMEM,
        scratch_shapes=[pltpu.VMEM(loss_mask.shape, loss_mask.dtype), pltpu.SemaphoreType.DMA((3,))],
        compiler_params=grant(2),
        name="prepare",
    )(keys, values, loss_mask)


def pack_kernel(w_ref, out_ref, sems):
    copies = []
    for g, block in enumerate(column_blocks(lax.axis_index("tensor") ^ 1)):
        at = pl.multiple_of(block * COLS, COLS)
        copies.append(pltpu.make_async_copy(w_ref.at[:, pl.ds(at, COLS)], out_ref.at[g], sems.at[g]))
        copies[-1].start()
    for copy in copies:
        copy.wait()


def pack(w):
    return pl.pallas_call(
        pack_kernel,
        out_shape=jax.ShapeDtypeStruct((8, w.shape[0], COLS), w.dtype),
        in_specs=[HBM],
        out_specs=HBM,
        scratch_shapes=[pltpu.SemaphoreType.DMA((8,))],
        compiler_params=grant(2),
        name="pack",
    )(w)


def attend(first_block, spans, blocks_refs, q8, lo_ref, m_ref, l_ref, acc, k_pair, v_pair, places, items):
    f32 = jnp.float32
    context = lax.axis_index("context")
    core = lax.rem(lax.axis_index("tensor"), NC)
    width = q8.shape[1]
    blocks = len(blocks_refs) * NZ
    for b in range(blocks):
        ref, at = blocks_refs[b // NZ], b % NZ * BLOCK
        k_pair[b] = ref[at : at + SPAN, :HD]
        v_pair[b] = ref[at : at + SPAN, HD:]
        places[b] = spans[gathered_slot(context, core, first_block + b)]
    places[blocks] = 1 << 20
    k_pair[blocks] = jnp.zeros((SPAN, HD), jnp.bfloat16)
    v_pair[blocks] = jnp.zeros((SPAN, HD), jnp.bfloat16)

    for i in range(2):
        first = jnp.min(lo_ref[i]).astype(jnp.int32)
        q_pos = spans[2 * context + i]
        count = jnp.int32(0)
        for b in range(blocks):
            items[count] = b
            seen = (places[b] <= q_pos) & ((places[b] + 1) * SPAN > first)
            count = count + seen.astype(jnp.int32)
        items[count] = blocks
        hi = lax.broadcasted_iota(jnp.int32, (SPAN, SPAN), 1) + q_pos * SPAN
        row = lax.broadcasted_iota(jnp.int32, (SPAN, SPAN), 0)

        def bias(place):
            pos = row + place * SPAN
            return jnp.where((pos.astype(f32) >= lo_ref[i]) & (pos <= hi), 0.0, LOW)

        def step(j, carry):
            b, c = items[2 * j], items[2 * j + 1]
            both = jnp.concatenate([bias(places[b]), bias(places[c])], axis=0)
            k = jnp.concatenate([k_pair[b], k_pair[c]], axis=0)
            v = jnp.concatenate([v_pair[b], v_pair[c]], axis=0)
            s = lax.dot_general(k, q8[i], (((1,), (1,)), ((), ())), preferred_element_type=f32)
            s = s * (HD ** (-0.5) * LOG2E) + jnp.concatenate([both] * (width // SPAN), axis=1)
            old = m_ref[i]
            new = jnp.maximum(old, jnp.max(s, axis=0, keepdims=True))
            alpha = jnp.exp2(old - new)
            p = jnp.exp2(s - new)
            m_ref[i] = new
            l_ref[i] = l_ref[i] * alpha + jnp.sum(p, axis=0, keepdims=True)
            add = lax.dot_general(
                v, p.astype(jnp.bfloat16), (((0,), (0,)), ((), ())), preferred_element_type=f32
            )
            acc[i] = acc[i] * alpha + add
            return carry

        lax.fori_loop(0, lax.shift_right_logical(count + 1, 1), step, 0)
    tally = jnp.zeros((TALLY, HD), f32)
    for ref in blocks_refs:
        for b in range(NZ):
            tally += ref[b * BLOCK + SPAN : (b + 1) * BLOCK, :HD].astype(f32)
    return tally


def first_kernel(
    spans, seg_ref, q_ref, q_other_ref, blocks_ref, q8, lo_ref, m_ref, l_ref, acc, tally_ref, k_pair, v_pair, places, items
):
    f32 = jnp.float32
    context = lax.axis_index("context")
    heads = q8.shape[1] // SPAN
    half = heads // 2
    seg = seg_ref[...]
    starts = [jnp.sum((seg < d).astype(f32), keepdims=True) for d in range(1, 8)]
    for i in range(2):
        for h in range(heads):
            ref = q_ref if h < half else q_other_ref
            q8[i, h * SPAN : (h + 1) * SPAN, :] = ref[i * SPAN : (i + 1) * SPAN, h % half * HD : (h % half + 1) * HD]
        q_seg = seg_ref[pl.ds(2 * context + i, 1), :]
        lo = jnp.zeros((1, SPAN), f32)
        for d in range(1, 8):
            lo = jnp.where(q_seg == d, starts[d - 1], lo)
        lo_ref[i] = lo
    m_ref[...] = jnp.full(m_ref.shape, LOW, f32)
    l_ref[...] = jnp.zeros(l_ref.shape, f32)
    acc[...] = jnp.zeros(acc.shape, f32)
    tally_ref[...] = attend(0, spans, (blocks_ref,), q8, lo_ref, m_ref, l_ref, acc, k_pair, v_pair, places, items)


def second_kernel(
    spans, a_ref, b_ref, q8, lo_ref, m_in, l_in, acc_in, tally_in, m_ref, l_ref, acc, tally_ref, k_pair, v_pair, places, items
):
    m_ref[...] = m_in[...]
    l_ref[...] = l_in[...]
    acc[...] = acc_in[...]
    tally = attend(NZ, spans, (a_ref, b_ref), q8, lo_ref, m_ref, l_ref, acc, k_pair, v_pair, places, items)
    tally_ref[...] = tally_in[...] + tally


def third_kernel(
    spans, blocks_ref, q8, lo_ref, m_in, l_in, acc_in, tally_in, out_ref, tally_ref, m_ref, l_ref, acc, k_pair, v_pair, places, items
):
    f32 = jnp.float32
    width = q8.shape[1]
    m_ref[...] = m_in[...]
    l_ref[...] = l_in[...]
    acc[...] = acc_in[...]
    tally = attend(3 * NZ, spans, (blocks_ref,), q8, lo_ref, m_ref, l_ref, acc, k_pair, v_pair, places, items)
    tally_ref[...] = tally_in[...] + tally
    row = lax.broadcasted_iota(jnp.int32, (TALLY, width), 0)
    for i in range(2):
        cols = slice(i * width, (i + 1) * width)
        total = l_ref[i]
        total = jnp.where(total > 0, total, 1.0)
        out_ref[:SPAN, cols] = (acc[i] / total).astype(jnp.bfloat16)
        log = m_ref[i] + jnp.log(total) * LOG2E
        high = log.astype(jnp.bfloat16).astype(f32)
        mid = (log - high).astype(jnp.bfloat16).astype(f32)
        tail = log - high - mid
        parts = jnp.where(row == 0, high, jnp.where(row == 1, mid, jnp.where(row == 2, tail, 0.0)))
        out_ref[SPAN:, cols] = parts.astype(jnp.bfloat16)


def attention(spans, seg, q, q_other, own, inner_blocks, outer_blocks, far_blocks):
    heads = 2 * q.shape[1] // HD
    width = heads * SPAN
    f32 = jnp.float32
    state = [((2, 1, width), f32), ((2, 1, width), f32), ((2, HD, width), f32)]
    tally = ((TALLY, HD), f32)

    def call(kernel, blocks, made, kept, *operands):
        return pl.pallas_call(
            kernel,
            out_shape=tuple(jax.ShapeDtypeStruct(*m) for m in made),
            in_specs=[SMEM] + [VMEM] * (len(operands) - 1),
            out_specs=(VMEM,) * len(made),
            scratch_shapes=[pltpu.VMEM(*m) for m in kept]
            + [
                pltpu.VMEM((blocks + 1, SPAN, HD), jnp.bfloat16),
                pltpu.VMEM((blocks + 1, SPAN, HD), jnp.bfloat16),
                pltpu.SMEM((blocks + 1,), jnp.int32),
                pltpu.SMEM((blocks + 2,), jnp.int32),
            ],
            compiler_params=grant(12),
        )(*operands)

    made = [((2, width, HD), jnp.bfloat16), ((2, 1, SPAN), f32), *state, tally]
    q8, lo, *running = call(first_kernel, NZ, made, [], spans, seg, q, q_other, own)
    running = call(second_kernel, 2 * NZ, [*state, tally], [], spans, inner_blocks, outer_blocks, q8, lo, *running)
    made = [((BLOCK, 2 * width), jnp.bfloat16), tally]
    return call(third_kernel, NZ, made, state, spans, far_blocks, q8, lo, *running)


def multiply(first, heads_ref, w_ref, other_ref, out_refs):
    depth = w_ref.shape[0]
    blocks = column_blocks(lax.axis_index("tensor"))
    for g, out_ref in enumerate(out_refs):
        at = pl.multiple_of(blocks[first + g] * COLS, COLS)
        total = jnp.dot(heads_ref[:, :depth], w_ref[:, pl.ds(at, COLS)], preferred_element_type=jnp.float32)
        total += jnp.dot(heads_ref[:, depth:], other_ref[first + g], preferred_element_type=jnp.float32)
        out_ref[...] = total.astype(jnp.bfloat16)


def join_kernel(mine_ref, theirs_ref, w_ref, other_ref, heads_ref, *out_refs):
    f32 = jnp.float32
    width = mine_ref.shape[1] // 2
    heads = width // SPAN

    def log(ref, at):
        rows = ref[SPAN:, at : at + SPAN].astype(f32)
        return rows[0:1] + rows[1:2] + rows[2:3]

    for i in range(2):
        for h in range(heads):
            a = i * width + h * SPAN
            b = i * width + (h + heads // 2) % heads * SPAN
            log_a, log_b = log(mine_ref, a), log(theirs_ref, b)
            top = jnp.maximum(log_a, log_b)
            part_a, part_b = jnp.exp2(log_a - top), jnp.exp2(log_b - top)
            total = part_a + part_b
            joined = mine_ref[:SPAN, a : a + SPAN].astype(f32) * (part_a / total)
            joined += theirs_ref[:SPAN, b : b + SPAN].astype(f32) * (part_b / total)
            heads_ref[i * SPAN : (i + 1) * SPAN, h * HD : (h + 1) * HD] = joined.T.astype(jnp.bfloat16)
    multiply(0, heads_ref, w_ref, other_ref, out_refs)


def join(mine, theirs, w, other):
    rows, depth = 2 * SPAN, 2 * w.shape[0]
    return pl.pallas_call(
        join_kernel,
        out_shape=(
            jax.ShapeDtypeStruct((rows, depth), jnp.bfloat16),
            jax.ShapeDtypeStruct((rows, COLS), jnp.bfloat16),
            jax.ShapeDtypeStruct((rows, COLS), jnp.bfloat16),
        ),
        in_specs=[VMEM] * 4,
        out_specs=(VMEM,) * 3,
        compiler_params=grant(20),
        name="join",
    )(mine, theirs, w, other)


def project_kernel(heads_ref, w_ref, other_ref, *out_refs):
    multiply(2, heads_ref, w_ref, other_ref, out_refs)


def project(heads, w, other):
    rows = heads.shape[0]
    return pl.pallas_call(
        project_kernel,
        out_shape=(jax.ShapeDtypeStruct((rows, COLS), jnp.bfloat16),) * 6,
        in_specs=[VMEM] * 3,
        out_specs=(VMEM,) * 6,
        compiler_params=grant(20),
        name="project",
    )(heads, w, other)


def add_kernel(a_ref, b_ref, out_ref):
    out_ref[...] = (a_ref[...].astype(jnp.float32) + b_ref[...].astype(jnp.float32)).astype(jnp.bfloat16)


def add(a, b):
    return pl.pallas_call(
        add_kernel,
        out_shape=jax.ShapeDtypeStruct(a.shape, a.dtype),
        in_specs=[VMEM, VMEM],
        out_specs=VMEM,
        compiler_params=grant(4),
        name="add",
    )(a, b)


def per_device(queries, keys, values, out_weight, segment_ids, loss_mask, span_order):
    both = ("context", "tensor")
    f32 = jnp.float32
    cat = lambda *a: jnp.concatenate(a, axis=0)
    in_hbm = lambda a: pltpu.with_memory_space_constraint(a, pltpu.HBM)

    kv1 = prepare(in_hbm(keys), in_hbm(values), in_hbm(loss_mask))
    r1 = lax.ppermute(kv1, both, perm_context("z", inner))
    q_other = lax.ppermute(queries[0], "tensor", SWAP)
    packed = pack(in_hbm(out_weight))
    kv2 = cat(kv1, r1)
    kv4 = cat(kv2, lax.ppermute(kv2, both, perm_context("z", outer)))
    weight_other = lax.ppermute(packed, "tensor", SWAP)
    beyond = lambda i, c, n: inner(outer(i, c, n), c, n)
    x_inner = lax.ppermute(kv4, both, perm_context("x", inner))
    x_outer = lax.ppermute(kv4, both, perm_context("x", outer))
    gathered = x_inner, x_outer, lax.ppermute(x_inner, both, perm_context("x", outer))
    mine, tally = attention(span_order, segment_ids.reshape(32, SPAN), queries[0], q_other, kv4, *gathered)
    theirs = lax.ppermute(mine, "tensor", SWAP)

    inward, outward = perm_tensor(inner), perm_tensor(outer)
    heads, far_a, far_b = join(mine, theirs, out_weight, weight_other)
    far_a = lax.ppermute(far_a, "tensor", outward)
    far_b = lax.ppermute(far_b, "tensor", outward)
    mid_a, mid_b, near_a, near_b, early, own = project(heads, out_weight, weight_other)
    around = [(d * 16 + t, (d + 1 + t % 2) % 3 * 16 + t) for d in range(3) for t in range(16)]
    early = lax.ppermute(early, "tensor", inward)
    one = lax.ppermute(tally, ("dp", "tensor"), around)
    two = lax.ppermute(one, "tensor", SWAP)
    mid_a = lax.ppermute(add(mid_a, far_a), "tensor", inward)
    mid_b = lax.ppermute(add(mid_b, far_b), "tensor", inward)
    near_a = lax.ppermute(add(near_a, mid_a), "tensor", perm_tensor(beyond))
    near_b = lax.ppermute(add(near_b, mid_b), "tensor", outward)
    count = (tally + one + two)[0, 0]
    scale_all = lax.axis_size("dp") * lax.axis_size("context") * queries.shape[1]
    weight = loss_mask[0].astype(f32) * scale_all / count
    summed = own.astype(f32) + early.astype(f32) + near_a.astype(f32) + near_b.astype(f32)
    return (summed * weight[:, None]).astype(jnp.bfloat16)[None]


def solution(mesh):
    in_specs = (
        P("dp", "context", "tensor"),
        P("dp", "context", None),
        P("dp", "context", None),
        P("tensor", None),
        P("dp", None),
        P("dp", "context"),
        P(),
    )
    out_specs = P("dp", "context", "tensor")
    return jax.shard_map(
        per_device, mesh=mesh, in_specs=in_specs, out_specs=out_specs, check_vma=False
    )
```

```python
import jax
import jax.numpy as jnp
from jax import lax
from jax.experimental import pallas as pl
from jax.experimental.pallas import tpu as pltpu
from jax.sharding import PartitionSpec as P


HD = 128
SPAN = 128
TALLY = 8
BLOCK = SPAN + TALLY
COLS = 512
LOG2E = 1.4426950408889634
LOW = -1e30


NX, NZ, NY, NC = 4, 4, 8, 2


def inner(i, c, n):
    return ((((i - c) & (n - 1)) ^ 1) + c) & (n - 1)


def outer(i, c, n):
    v = (i - c) & (n - 1)
    return (v + 2 * (v & 1) - 1 + c) & (n - 1)


def perm_context(axis, partner):
    out = []
    for x in range(NX):
        for z in range(NZ):
            for y in range(NY):
                for c in range(NC):
                    px = partner(x, c, NX) if axis == "x" else x
                    pz = partner(z, c, NZ) if axis == "z" else z
                    tensor = y * NC + c
                    out.append(((x * NZ + z) * 16 + tensor, (px * NZ + pz) * 16 + tensor))
    return out


def perm_tensor(partner):
    return [
        (y * NC + c, partner(y, c, NY) * NC + c) for y in range(NY) for c in range(NC)
    ]


SWAP = [(t, t ^ 1) for t in range(16)]


def gathered_slot(context, core, i):
    def known(at, n):
        far = outer(at, core, n)
        return (at, inner(at, core, n), far, inner(far, core, n))

    x = known(context >> 2, NX)[i // NZ]
    z = known(context & (NZ - 1), NZ)[i % NZ]
    return 2 * (x * NZ + z) + core


def column_blocks(tensor):
    y, core = tensor >> 1, tensor & 1
    v = (y - core) & (NY - 1)
    k, s = v >> 1, v & 1
    far, mid, near = (k + 2) & 3, (k + 1 - 2 * s) & 3, (k - 1 + 2 * s) & 3
    order = (2 * far + s, 2 * far + 1 - s, 2 * mid + 1 - s, 2 * mid + s)
    order += (2 * near + s, 2 * near + 1 - s, 2 * k + 1 - s, 2 * k + s)
    return [2 * ((b + core) & (NY - 1)) + core for b in order]


SMEM = pl.BlockSpec(memory_space=pltpu.SMEM)
VMEM = pl.BlockSpec(memory_space=pltpu.VMEM)
HBM = pl.BlockSpec(memory_space=pltpu.HBM)


def grant(mib):
    return pltpu.CompilerParams(vmem_limit_bytes=mib * 2**20)


def prepare_kernel(k_ref, v_ref, mask_hbm, out_ref, mask_ref, sems):
    counted = pltpu.make_async_copy(mask_hbm, mask_ref, sems.at[2])
    counted.start()
    tensor = lax.axis_index("tensor")
    rows = pl.ds(pl.multiple_of(lax.rem(tensor, NC) * SPAN, SPAN), SPAN)
    cols = pl.ds(pl.multiple_of(lax.div(tensor, NC) * HD, HD), HD)
    copies = []
    for i, ref in enumerate((k_ref, v_ref)):
        into = out_ref.at[pl.ds(0, SPAN), pl.ds(i * HD, HD)]
        copies.append(pltpu.make_async_copy(ref.at[0, rows, cols], into, sems.at[i]))
        copies[-1].start()
    counted.wait()
    total = jnp.sum(mask_ref[...].astype(jnp.float32), axis=1, keepdims=True)
    out_ref[SPAN:, :] = jnp.broadcast_to(total, (TALLY, 2 * HD)).astype(jnp.bfloat16)
    for copy in copies:
        copy.wait()


def prepare(keys, values, loss_mask):
    return pl.pallas_call(
        prepare_kernel,
        out_shape=jax.ShapeDtypeStruct((BLOCK, 2 * HD), jnp.bfloat16),
        in_specs=[HBM] * 3,
        out_specs=VMEM,
        scratch_shapes=[pltpu.VMEM(loss_mask.shape, loss_mask.dtype), pltpu.SemaphoreType.DMA((3,))],
        compiler_params=grant(2),
        name="prepare",
    )(keys, values, loss_mask)


def pack_kernel(w_ref, out_ref, sems):
    copies = []
    for g, block in enumerate(column_blocks(lax.axis_index("tensor") ^ 1)):
        at = pl.multiple_of(block * COLS, COLS)
        copies.append(pltpu.make_async_copy(w_ref.at[:, pl.ds(at, COLS)], out_ref.at[g], sems.at[g]))
        copies[-1].start()
    for copy in copies:
        copy.wait()


def pack(w):
    return pl.pallas_call(
        pack_kernel,
        out_shape=jax.ShapeDtypeStruct((8, w.shape[0], COLS), w.dtype),
        in_specs=[HBM],
        out_specs=HBM,
        scratch_shapes=[pltpu.SemaphoreType.DMA((8,))],
        compiler_params=grant(2),
        name="pack",
    )(w)


def attend(first_block, spans, blocks_refs, q8, lo_ref, m_ref, l_ref, acc, k_pair, v_pair, places, items):
    f32 = jnp.float32
    context = lax.axis_index("context")
    core = lax.rem(lax.axis_index("tensor"), NC)
    width = q8.shape[1]
    blocks = len(blocks_refs) * NZ
    for b in range(blocks):
        ref, at = blocks_refs[b // NZ], b % NZ * BLOCK
        k_pair[b] = ref[at : at + SPAN, :HD]
        v_pair[b] = ref[at : at + SPAN, HD:]
        places[b] = spans[gathered_slot(context, core, first_block + b)]
    places[blocks] = 1 << 20
    k_pair[blocks] = jnp.zeros((SPAN, HD), jnp.bfloat16)
    v_pair[blocks] = jnp.zeros((SPAN, HD), jnp.bfloat16)

    for i in range(2):
        first = jnp.min(lo_ref[i]).astype(jnp.int32)
        q_pos = spans[2 * context + i]
        count = jnp.int32(0)
        for b in range(blocks):
            items[count] = b
            seen = (places[b] <= q_pos) & ((places[b] + 1) * SPAN > first)
            count = count + seen.astype(jnp.int32)
        items[count] = blocks
        hi = lax.broadcasted_iota(jnp.int32, (SPAN, SPAN), 1) + q_pos * SPAN
        row = lax.broadcasted_iota(jnp.int32, (SPAN, SPAN), 0)

        def bias(place):
            pos = row + place * SPAN
            return jnp.where((pos.astype(f32) >= lo_ref[i]) & (pos <= hi), 0.0, LOW)

        def step(j, carry):
            b, c = items[2 * j], items[2 * j + 1]
            both = jnp.concatenate([bias(places[b]), bias(places[c])], axis=0)
            k = jnp.concatenate([k_pair[b], k_pair[c]], axis=0)
            v = jnp.concatenate([v_pair[b], v_pair[c]], axis=0)
            s = lax.dot_general(k, q8[i], (((1,), (1,)), ((), ())), preferred_element_type=f32)
            s = s * (HD ** (-0.5) * LOG2E) + jnp.concatenate([both] * (width // SPAN), axis=1)
            old = m_ref[i]
            new = jnp.maximum(old, jnp.max(s, axis=0, keepdims=True))
            alpha = jnp.exp2(old - new)
            p = jnp.exp2(s - new)
            m_ref[i] = new
            l_ref[i] = l_ref[i] * alpha + jnp.sum(p, axis=0, keepdims=True)
            add = lax.dot_general(
                v, p.astype(jnp.bfloat16), (((0,), (0,)), ((), ())), preferred_element_type=f32
            )
            acc[i] = acc[i] * alpha + add
            return carry

        lax.fori_loop(0, lax.shift_right_logical(count + 1, 1), step, 0)
    tally = jnp.zeros((TALLY, HD), f32)
    for ref in blocks_refs:
        for b in range(NZ):
            tally += ref[b * BLOCK + SPAN : (b + 1) * BLOCK, :HD].astype(f32)
    return tally


def first_kernel(
    spans, seg_ref, q_ref, q_other_ref, blocks_ref, q8, lo_ref, m_ref, l_ref, acc, tally_ref, k_pair, v_pair, places, items
):
    f32 = jnp.float32
    context = lax.axis_index("context")
    heads = q8.shape[1] // SPAN
    half = heads // 2
    seg = seg_ref[...]
    starts = [jnp.sum((seg < d).astype(f32), keepdims=True) for d in range(1, 8)]
    for i in range(2):
        for h in range(heads):
            ref = q_ref if h < half else q_other_ref
            q8[i, h * SPAN : (h + 1) * SPAN, :] = ref[i * SPAN : (i + 1) * SPAN, h % half * HD : (h % half + 1) * HD]
        q_seg = seg_ref[pl.ds(2 * context + i, 1), :]
        lo = jnp.zeros((1, SPAN), f32)
        for d in range(1, 8):
            lo = jnp.where(q_seg == d, starts[d - 1], lo)
        lo_ref[i] = lo
    m_ref[...] = jnp.full(m_ref.shape, LOW, f32)
    l_ref[...] = jnp.zeros(l_ref.shape, f32)
    acc[...] = jnp.zeros(acc.shape, f32)
    tally_ref[...] = attend(0, spans, (blocks_ref,), q8, lo_ref, m_ref, l_ref, acc, k_pair, v_pair, places, items)


def second_kernel(
    spans, a_ref, b_ref, q8, lo_ref, m_in, l_in, acc_in, tally_in, m_ref, l_ref, acc, tally_ref, k_pair, v_pair, places, items
):
    m_ref[...] = m_in[...]
    l_ref[...] = l_in[...]
    acc[...] = acc_in[...]
    tally = attend(NZ, spans, (a_ref, b_ref), q8, lo_ref, m_ref, l_ref, acc, k_pair, v_pair, places, items)
    tally_ref[...] = tally_in[...] + tally


def third_kernel(
    spans, blocks_ref, q8, lo_ref, m_in, l_in, acc_in, tally_in, out_ref, tally_ref, m_ref, l_ref, acc, k_pair, v_pair, places, items
):
    f32 = jnp.float32
    width = q8.shape[1]
    m_ref[...] = m_in[...]
    l_ref[...] = l_in[...]
    acc[...] = acc_in[...]
    tally = attend(3 * NZ, spans, (blocks_ref,), q8, lo_ref, m_ref, l_ref, acc, k_pair, v_pair, places, items)
    tally_ref[...] = tally_in[...] + tally
    row = lax.broadcasted_iota(jnp.int32, (TALLY, width), 0)
    for i in range(2):
        cols = slice(i * width, (i + 1) * width)
        total = l_ref[i]
        total = jnp.where(total > 0, total, 1.0)
        out_ref[:SPAN, cols] = (acc[i] / total).astype(jnp.bfloat16)
        log = m_ref[i] + jnp.log(total) * LOG2E
        high = log.astype(jnp.bfloat16).astype(f32)
        mid = (log - high).astype(jnp.bfloat16).astype(f32)
        tail = log - high - mid
        parts = jnp.where(row == 0, high, jnp.where(row == 1, mid, jnp.where(row == 2, tail, 0.0)))
        out_ref[SPAN:, cols] = parts.astype(jnp.bfloat16)


def attention(spans, seg, q, q_other, own, inner_blocks, outer_blocks, far_blocks):
    heads = 2 * q.shape[1] // HD
    width = heads * SPAN
    f32 = jnp.float32
    state = [((2, 1, width), f32), ((2, 1, width), f32), ((2, HD, width), f32)]
    tally = ((TALLY, HD), f32)

    def call(kernel, blocks, made, kept, *operands):
        return pl.pallas_call(
            kernel,
            out_shape=tuple(jax.ShapeDtypeStruct(*m) for m in made),
            in_specs=[SMEM] + [VMEM] * (len(operands) - 1),
            out_specs=(VMEM,) * len(made),
            scratch_shapes=[pltpu.VMEM(*m) for m in kept]
            + [
                pltpu.VMEM((blocks + 1, SPAN, HD), jnp.bfloat16),
                pltpu.VMEM((blocks + 1, SPAN, HD), jnp.bfloat16),
                pltpu.SMEM((blocks + 1,), jnp.int32),
                pltpu.SMEM((blocks + 2,), jnp.int32),
            ],
            compiler_params=grant(12),
        )(*operands)

    made = [((2, width, HD), jnp.bfloat16), ((2, 1, SPAN), f32), *state, tally]
    q8, lo, *running = call(first_kernel, NZ, made, [], spans, seg, q, q_other, own)
    running = call(second_kernel, 2 * NZ, [*state, tally], [], spans, inner_blocks, outer_blocks, q8, lo, *running)
    made = [((BLOCK, 2 * width), jnp.bfloat16), tally]
    return call(third_kernel, NZ, made, state, spans, far_blocks, q8, lo, *running)


def multiply(first, heads_ref, w_ref, other_ref, out_refs):
    depth = w_ref.shape[0]
    blocks = column_blocks(lax.axis_index("tensor"))
    for g, out_ref in enumerate(out_refs):
        at = pl.multiple_of(blocks[first + g] * COLS, COLS)
        total = jnp.dot(heads_ref[:, :depth], w_ref[:, pl.ds(at, COLS)], preferred_element_type=jnp.float32)
        total += jnp.dot(heads_ref[:, depth:], other_ref[first + g], preferred_element_type=jnp.float32)
        out_ref[...] = total.astype(jnp.bfloat16)


def join_kernel(mine_ref, theirs_ref, w_ref, other_ref, heads_ref, *out_refs):
    f32 = jnp.float32
    width = mine_ref.shape[1] // 2
    heads = width // SPAN

    def log(ref, at):
        rows = ref[SPAN:, at : at + SPAN].astype(f32)
        return rows[0:1] + rows[1:2] + rows[2:3]

    for i in range(2):
        for h in range(heads):
            a = i * width + h * SPAN
            b = i * width + (h + heads // 2) % heads * SPAN
            log_a, log_b = log(mine_ref, a), log(theirs_ref, b)
            top = jnp.maximum(log_a, log_b)
            part_a, part_b = jnp.exp2(log_a - top), jnp.exp2(log_b - top)
            total = part_a + part_b
            joined = mine_ref[:SPAN, a : a + SPAN].astype(f32) * (part_a / total)
            joined += theirs_ref[:SPAN, b : b + SPAN].astype(f32) * (part_b / total)
            heads_ref[i * SPAN : (i + 1) * SPAN, h * HD : (h + 1) * HD] = joined.T.astype(jnp.bfloat16)
    multiply(0, heads_ref, w_ref, other_ref, out_refs)


def join(mine, theirs, w, other):
    rows, depth = 2 * SPAN, 2 * w.shape[0]
    return pl.pallas_call(
        join_kernel,
        out_shape=(
            jax.ShapeDtypeStruct((rows, depth), jnp.bfloat16),
            jax.ShapeDtypeStruct((rows, COLS), jnp.bfloat16),
            jax.ShapeDtypeStruct((rows, COLS), jnp.bfloat16),
        ),
        in_specs=[VMEM] * 4,
        out_specs=(VMEM,) * 3,
        compiler_params=grant(20),
        name="join",
    )(mine, theirs, w, other)


def project_kernel(heads_ref, w_ref, other_ref, *out_refs):
    multiply(2, heads_ref, w_ref, other_ref, out_refs)


def project(heads, w, other):
    rows = heads.shape[0]
    return pl.pallas_call(
        project_kernel,
        out_shape=(jax.ShapeDtypeStruct((rows, COLS), jnp.bfloat16),) * 6,
        in_specs=[VMEM] * 3,
        out_specs=(VMEM,) * 6,
        compiler_params=grant(20),
        name="project",
    )(heads, w, other)


def add_kernel(a_ref, b_ref, *refs):
    *beside, out_ref = refs
    total = a_ref[...].astype(jnp.float32) + b_ref[0].astype(jnp.float32)
    out_ref[0] = total.astype(jnp.bfloat16)
    for i, ref in enumerate(beside):
        out_ref[1 + i] = ref[...]


def add(a, b, *beside):
    return pl.pallas_call(
        add_kernel,
        out_shape=jax.ShapeDtypeStruct((1 + len(beside), *a.shape), a.dtype),
        in_specs=[VMEM] * (2 + len(beside)),
        out_specs=VMEM,
        compiler_params=grant(4),
        name="add",
    )(a, b, *beside)


def per_device(queries, keys, values, out_weight, segment_ids, loss_mask, span_order):
    both = ("context", "tensor")
    f32 = jnp.float32
    cat = lambda *a: jnp.concatenate(a, axis=0)
    in_hbm = lambda a: pltpu.with_memory_space_constraint(a, pltpu.HBM)

    kv1 = prepare(in_hbm(keys), in_hbm(values), in_hbm(loss_mask))
    r1 = lax.ppermute(kv1, both, perm_context("z", inner))
    q_other = lax.ppermute(queries[0], "tensor", SWAP)
    packed = pack(in_hbm(out_weight))
    kv2 = cat(kv1, r1)
    kv4 = cat(kv2, lax.ppermute(kv2, both, perm_context("z", outer)))
    weight_other = lax.ppermute(packed, "tensor", SWAP)
    beyond = lambda i, c, n: inner(outer(i, c, n), c, n)
    x_inner = lax.ppermute(kv4, both, perm_context("x", inner))
    x_outer = lax.ppermute(kv4, both, perm_context("x", outer))
    gathered = x_inner, x_outer, lax.ppermute(x_inner, both, perm_context("x", outer))
    mine, tally = attention(span_order, segment_ids.reshape(32, SPAN), queries[0], q_other, kv4, *gathered)
    theirs = lax.ppermute(mine, "tensor", SWAP)

    inward, outward = perm_tensor(inner), perm_tensor(outer)
    heads, far_a, far_b = join(mine, theirs, out_weight, weight_other)
    far_a = lax.ppermute(far_a, "tensor", outward)
    far_b = lax.ppermute(far_b, "tensor", outward)
    mid_a, mid_b, near_a, near_b, beside, own = project(heads, out_weight, weight_other)
    around = [(d * 16 + t, (d + 1 + t % 2) % 3 * 16 + t) for d in range(3) for t in range(16)]
    one = lax.ppermute(tally, ("dp", "tensor"), around)
    two = lax.ppermute(one, "tensor", SWAP)
    mid_a = lax.ppermute(add(mid_a, far_a[None]), "tensor", inward)
    mid_b = lax.ppermute(add(mid_b, far_b[None], beside), "tensor", inward)
    near_a = lax.ppermute(add(near_a, mid_a), "tensor", perm_tensor(beyond))
    near_b = lax.ppermute(add(near_b, mid_b), "tensor", outward)
    count = (tally + one + two)[0, 0]
    scale_all = lax.axis_size("dp") * lax.axis_size("context") * queries.shape[1]
    weight = loss_mask[0].astype(f32) * scale_all / count
    summed = own.astype(f32) + mid_b[1].astype(f32) + near_a[0].astype(f32) + near_b[0].astype(f32)
    return (summed * weight[:, None]).astype(jnp.bfloat16)[None]


def solution(mesh):
    in_specs = (
        P("dp", "context", "tensor"),
        P("dp", "context", None),
        P("dp", "context", None),
        P("tensor", None),
        P("dp", None),
        P("dp", "context"),
        P(),
    )
    out_specs = P("dp", "context", "tensor")
    return jax.shard_map(
        per_device, mesh=mesh, in_specs=in_specs, out_specs=out_specs, check_vma=False
    )
```
